128 devices in a mesh: gx: 8 (over z, core), gy: 16 (over x, y).
Axes of the slice: x: 4, y: 4, z: 4, core: 2. Of those that a mesh axis runs over, the one named last changes fastest.
Arguments:
- prolong: bfloat16 [8192, 24, 128], P(('gx', 'gy')), may hold values from -0.5 to 0.5
- stiffness: bfloat16 [16384, 4, 128, 128], P(('gx', 'gy')), may hold values from -6 to 6
- request: int32 [16384], P(('gx', 'gy')), may hold values from 0 to 63, as said below
- col_slot: int32 [16384, 4], P(('gx', 'gy')), may hold values from 0 to 127
- col_pos: int32 [16384, 4], P(('gx', 'gy')), may hold values from 0 to 15, as said below
- coarse_owner: int32 [8192, 1], P(('gx', 'gy')), may hold values from 0 to 127; in each aligned block of 64 rows (0 to 63, 64 to 127, ...) no two rows name the same one
Outputs:
- coarse: float32 [16384, 24, 384], P(('gx', 'gy'))
The draws below stay inside these ranges and needn't reach their ends.
Inputs may be any that keep to these rules, and one draw needn't show every extreme that they name: `request`: on each device, entries k * 1 to (k + 1) * 1 - 1 name distinct aggregates of device k, as local indices there. `col_pos`: the 4 entries of one block row are distinct. `coarse_owner`: among one device's 64 aggregates at most 1 share a coarse owner, and on some devices 1 do.
All inputs are finite; a program needn't handle non-finite values.
Results may differ from the reference program's by a relative error of at most 0.0003.
Values may be sent and summed in bfloat16 or wider, within the bound.
A program may use at most 128 MiB of HBM per device.

```python
import math
import jax
import jax.numpy as jnp
import numpy as np
from jax import lax

AGG_DEV = 64
DOF = 128
CV = 24
MAXNB = 16
SLOT_DEV = 128
BPS = 4
SEND_MAX = 1
IN_ROWS = 128
NAGG = 8192
SLOTS = 16384
DEVICES = 128


def draw_request(key, part):
    per_peer = SLOT_DEV // DEVICES
    scores = jax.random.randint(key, (DEVICES * DEVICES, AGG_DEV), 0, 1 << 20) * AGG_DEV
    scores = scores + jnp.arange(AGG_DEV, dtype=jnp.int32)[None, :]
    chosen = jnp.argsort(scores, axis=1)[:, :per_peer]
    return chosen.reshape(-1).astype(jnp.int32)


def draw_col_pos(key, part):
    scores = jax.random.randint(key, (DEVICES * SLOT_DEV, MAXNB), 0, 1 << 20) * MAXNB
    scores = scores + jnp.arange(MAXNB, dtype=jnp.int32)[None, :]
    chosen = jnp.argsort(scores, axis=1)[:, :BPS]
    return chosen.astype(jnp.int32)


def touch_ends(values, key, low, high):
    longest = values.shape.index(max(values.shape))
    spots = []
    for shift in (0, 1):
        where = [jax.random.randint(jax.random.fold_in(key, axis), (), 0, length) for axis, length in enumerate(values.shape)]
        where[longest] = (where[longest] + shift) % values.shape[longest]
        spots.append(tuple(where))
    return values.at[spots[0]].set(low).at[spots[1]].set(high)


def level_of(own_key, shape, cuts, low, high):
    def one(position, shards_of):
        draws = jax.random.uniform(jax.random.fold_in(jax.random.fold_in(own_key, 6), position), (shards_of,), jnp.float32, low / len(cuts), high / len(cuts))
        return jnp.repeat(jnp.exp(draws), shape[position] // shards_of).reshape((-1,) + (1,) * (len(shape) - position - 1))

    factor_of = one(*cuts[0])
    for cut in cuts[1:]:
        factor_of = factor_of * one(*cut)
    return factor_of


def deal_out(stream_key, own, number, rows, count, top, reach, lean):
    order = jax.random.permutation(stream_key, count)
    heavy_load, common = load_shares(count, rows * top, reach, lean, True), load_shares(count, rows * top, reach, lean, False)
    places = jnp.arange(count)

    def named(sizes, offset_by):
        used = int((sizes > 0).sum())
        fixed = max(1, used // 4)
        shifted = fixed + (places - fixed + offset_by * (used - fixed)) % max(1, count - fixed)
        return jnp.zeros((count,), jnp.int32).at[order[jnp.where(places < fixed, places, shifted)]].set(jnp.asarray(sizes, jnp.int32))

    sizes = jnp.where(number % 4 == 0, named(heavy_load, number // 4), named(common, number - number // 4 - 1))
    mixed = jax.random.permutation(jax.random.fold_in(own, 3), count)
    source_of, taker = mixed[0:count // 2 * 2:2], mixed[1:count // 2 * 2:2]
    room = jnp.minimum(sizes[source_of] - 1, reach - sizes[taker]) // 2
    room = jnp.where((source_of == order[0]) | (taker == order[0]) | (sizes[taker] == 0), 0, jnp.maximum(room, 0))
    shifted = jax.random.randint(jax.random.fold_in(own, 4), (count // 2,), 0, 1 << 20) % (room + 1)
    sizes = sizes.at[source_of].add(-shifted).at[taker].add(shifted)
    items = jnp.searchsorted(jnp.cumsum(sizes), jnp.arange(rows * top), side="right").astype(jnp.int32)
    listing = items.reshape(top, rows).T
    listing = listing[jax.random.permutation(jax.random.fold_in(own, 1), rows)]
    offset_by = jax.random.randint(jax.random.fold_in(own, 2), (rows, 1), 0, top)
    return jnp.take_along_axis(listing, (jnp.arange(top)[None, :] + offset_by) % top, axis=1)


def load_shares(count, total, reach, slope, full):
    portions = [(1 << 20) // math.isqrt(rank ** slope) + 1 for rank in range(1, count + 1)]
    largest = reach if full else min(reach, max(-(-total // count), total * portions[0] // sum(portions)))
    least = 1 if total - largest >= count - 1 else 0
    holding, rest = [largest] + [least] * (count - 1), total - largest - least * (count - 1)
    while rest > 0:
        candidates = [i for i in range(1, count) if holding[i] < largest] or [i for i in range(1, count) if holding[i] < reach]
        whole, budget = sum([portions[i] for i in candidates]), rest
        for i in candidates:
            addition = min(reach - holding[i], max(1, budget * portions[i] // whole), rest)
            holding[i] = holding[i] + addition
            rest = rest - addition
    return np.array(holding)


def bell_draw(own_key, extent, width, limit, shards=(), held_as=jnp.bfloat16):
    values = width * jax.random.normal(own_key, extent, jnp.float32)
    if shards:
        values = values * level_of(own_key, extent, shards, -0.22, 0.18)
    return jnp.clip(values, -limit, limit).astype(held_as)


def setup_inputs(seed: int = 0) -> dict:
    arg_keys = jax.random.split(jax.random.key(seed), 7)
    prolong = bell_draw(arg_keys[0], (NAGG, CV, DOF), DOF ** -0.5, 0.5, ((0, 128),))
    stiffness = bell_draw(arg_keys[1], (SLOTS, BPS, DOF, DOF), 1.0, 6.0, ((0, 128),))
    request = draw_request(jax.random.fold_in(arg_keys[6], 71), 0)
    col_slot = touch_ends(jax.random.randint(arg_keys[3], (SLOTS, BPS), 0, SLOT_DEV), jax.random.fold_in(arg_keys[3], 1), 0, SLOT_DEV - 1).astype(jnp.int32)
    col_pos = draw_col_pos(jax.random.fold_in(arg_keys[6], 71), 0)
    coarse_owner_keys = jax.random.split(jax.random.fold_in(arg_keys[5], 1), NAGG // AGG_DEV)
    coarse_owner_turns = jax.random.permutation(jax.random.fold_in(arg_keys[5], 3), NAGG // AGG_DEV)
    coarse_owner = jax.vmap(lambda own, number: deal_out(jax.random.fold_in(arg_keys[5], 2), own, number, AGG_DEV, DEVICES, 1, SEND_MAX, 2))(coarse_owner_keys, coarse_owner_turns).reshape((NAGG, 1))
    return {"prolong": prolong, "stiffness": stiffness, "request": request, "col_slot": col_slot, "col_pos": col_pos, "coarse_owner": coarse_owner}


HIGH = lax.Precision.HIGHEST


def device_rows(prolong, stiff_block, request_block, slot_block, pos_block):
    per_peer = SLOT_DEV // DEVICES
    gid = (jnp.arange(SLOT_DEV, dtype=jnp.int32) // per_peer) * AGG_DEV + request_block.astype(jnp.int32)
    fetched = prolong[gid].astype(jnp.float32)
    col_rows = fetched[slot_block]
    applied = jnp.einsum("tqij,tqej->tqei", stiff_block.astype(jnp.float32), col_rows, precision=HIGH)
    partial_value = jnp.einsum("tci,tqei->tqce", fetched, applied, precision=HIGH)
    column_hot = (pos_block[:, :, None] == jnp.arange(MAXNB, dtype=jnp.int32)[None, None, :]).astype(jnp.float32)
    spread = jnp.einsum("tqce,tqn->tcne", partial_value, column_hot, precision=HIGH)
    return gid, spread.reshape(SLOT_DEV, CV, MAXNB * CV)


def reference(prolong, stiffness, request, col_slot, col_pos, coarse_owner):
    stiff_dev = stiffness.reshape(DEVICES, SLOT_DEV, BPS, DOF, DOF)
    request_dev = request.reshape(DEVICES, SLOT_DEV)
    slot_dev = col_slot.reshape(DEVICES, SLOT_DEV, BPS)
    pos_dev = col_pos.reshape(DEVICES, SLOT_DEV, BPS)

    def accumulate(total, pieces):
        gid, spread = device_rows(prolong, pieces[0], pieces[1], pieces[2], pieces[3])
        return total.at[gid].add(spread), None

    start = jnp.zeros((NAGG, CV, MAXNB * CV), jnp.float32)
    fine_coarse, _ = lax.scan(accumulate, start, (stiff_dev, request_dev, slot_dev, pos_dev))
    owners = coarse_owner[:, 0].reshape(DEVICES, AGG_DEV)
    peer_ids = jnp.arange(DEVICES, dtype=jnp.int32)
    owner_one = (owners[:, :, None] == peer_ids[None, None, :]).astype(jnp.int32)
    before = jnp.cumsum(owner_one, axis=1) - owner_one
    row_rank = jnp.sum(before * owner_one, axis=2)
    source = jnp.arange(DEVICES, dtype=jnp.int32)[:, None]
    target = (owners * IN_ROWS + source * SEND_MAX + row_rank).reshape(-1).astype(jnp.int32)
    coarse = jnp.zeros((DEVICES * IN_ROWS, CV, MAXNB * CV), jnp.float32).at[target].set(fine_coarse)
    return coarse
```

```python
import functools

import jax
import jax.numpy as jnp
from jax import lax
from jax.experimental import pallas as pl
from jax.experimental.pallas import tpu as pltpu
from jax.sharding import PartitionSpec as P

MAXNB = 16
AXES = ("gx", "gy")
LANES = 128
SPAN = 32
ROUNDS = 16
WIDE = 8
TOP = 32767.0
MESH = pl.DeviceIdType.MESH
HBM = pl.BlockSpec(memory_space=pl.ANY)
VMEM = pl.BlockSpec(memory_space=pltpu.VMEM)
SMEM = pl.BlockSpec(memory_space=pltpu.SMEM)
NT = (((1,), (1,)), ((), ()))


def as_row(column):
    rows = column.shape[0]
    shape = (rows, LANES)
    eye = lax.broadcasted_iota(jnp.int32, shape, 0) == lax.broadcasted_iota(jnp.int32, shape, 1)
    return jnp.sum(jnp.where(eye, column, 0.0), axis=0, keepdims=True)


def as_column(row, rows):
    shape = (rows, LANES)
    eye = lax.broadcasted_iota(jnp.int32, shape, 0) == lax.broadcasted_iota(jnp.int32, shape, 1)
    return jnp.sum(jnp.where(eye, row, 0.0), axis=1, keepdims=True)


def coded(values):
    top = jnp.maximum(jnp.max(jnp.abs(values), axis=1, keepdims=True), 1e-30)
    code = jnp.round(values * (TOP / top)).astype(jnp.int32).astype(jnp.int16)
    return code, top * (1.0 / TOP)


def split(values):
    hi = values.astype(jnp.bfloat16)
    return hi, (values - hi.astype(jnp.float32)).astype(jnp.bfloat16)


def whole_kernel(
    slot_ref, owner_ref, meta_ref, prolong_ref, stiff_ref,
    out_ref,
    meta_in, req_ref, stage_ref, fetched_ref, mats_ref, pk_ref, cols_ref,
    code_ref, factor_ref, part_ref, scale_ref, spread_ref, total_ref,
    rows_ref, rows_scale, land_ref, land_scale, wide_ref,
    meta_send, meta_recv, fetch_send, fetch_recv, part_send, part_recv, fact_send, fact_recv,
    rows_send, rows_recv, rsc_send, rsc_recv, mats_sem, req_sem, out_sem,
):
    n, cv, dof = fetched_ref.shape
    bps = mats_ref.shape[1]
    width = out_ref.shape[2]
    gx, gy = lax.axis_index("gx"), lax.axis_index("gy")
    me = gx * 16 + gy
    z, core = gx // 2, lax.rem(gx, 2)
    x, y = gy // 4, lax.rem(gy, 4)
    to_gx = [lax.rem(z + j // 2, 4) * 2 + lax.rem(core + j, 2) for j in range(WIDE)]
    from_gx = [lax.rem(z + 4 - j // 2, 4) * 2 + lax.rem(core + j, 2) for j in range(WIDE)]

    def target(i, j):
        s = lax.rem(i * 5 + j * 3, 16)
        return to_gx[j], lax.rem(x + s // 4, 4) * 4 + lax.rem(y + s, 4)

    def source(i, j):
        s = lax.rem(i * 5 + j * 3, 16)
        return from_gx[j] * 16 + lax.rem(x + 4 - s // 4, 4) * 4 + lax.rem(y + 16 - s, 4)

    def each(fn):
        def body(i, c):
            for j in range(WIDE):
                fn(i, j)
            return c

        for j in range(1, WIDE):
            fn(0, j)
        lax.fori_loop(1, ROUNDS, body, 0)

    def remote(src, dst, send_sem, recv_sem, where):
        return pltpu.make_async_remote_copy(
            src_ref=src, dst_ref=dst, send_sem=send_sem, recv_sem=recv_sem,
            device_id=where, device_id_type=MESH,
        )

    def bulk(src, dst, send_sem, recv_sem, count):
        return remote(
            src.at[pl.ds(0, count)], dst.at[pl.ds(0, count)], send_sem, recv_sem, (gx, gy)
        )

    loads = [
        pltpu.make_async_copy(
            stiff_ref.at[pl.ds(b * 16, 16)], mats_ref.at[pl.ds(b * 16, 16)], mats_sem.at[b]
        )
        for b in range(n // 16)
    ]
    for copy in loads:
        copy.start()

    barrier = pltpu.get_barrier_semaphore()

    def greet(i, j):
        pl.semaphore_signal(barrier, inc=1, device_id=target(i, j), device_id_type=MESH)

    each(greet)
    meta_in[me] = meta_ref[me]
    cols_ref[...] = jnp.zeros_like(cols_ref)
    pl.semaphore_wait(barrier, n - 1)

    def ask(i, j):
        where = target(i, j)
        remote(
            meta_ref.at[where[0] * 16 + where[1]], meta_in.at[me],
            meta_send.at[0], meta_recv.at[0], where,
        ).start()

    each(ask)
    bulk(meta_ref, meta_in, meta_send.at[0], meta_recv.at[0], n - 1).wait()
    to_scalars = pltpu.make_async_copy(meta_in, req_ref, req_sem.at[0])
    to_scalars.start()
    to_scalars.wait()

    def fill(p, c):
        stage_ref[p] = prolong_ref[req_ref[p, 0, 0]]
        return c

    lax.fori_loop(0, n, fill, 0, unroll=8)

    def answer(i, j):
        where = target(i, j)
        remote(
            stage_ref.at[where[0] * 16 + where[1]], fetched_ref.at[me],
            fetch_send.at[0], fetch_recv.at[i], where,
        ).start()

    each(answer)
    fetched_ref[me] = prolong_ref[req_ref[me, 0, 0]]
    for copy in loads:
        copy.wait()

    def left_product(t):
        rows = fetched_ref[t]
        for h in range(bps // 2):
            pair = jnp.concatenate([mats_ref[t, 2 * h], mats_ref[t, 2 * h + 1]], axis=1)
            prod = jnp.dot(rows, pair, preferred_element_type=jnp.float32)
            hi, lo = split(prod)
            for u in range(2):
                at = slice(u * dof, (u + 1) * dof)
                pk_ref[t, 2 * h + u, :, 0:dof] = hi[:, at]
                pk_ref[t, 2 * h + u, :, dof : 2 * dof] = lo[:, at]

    bulk(stage_ref, fetched_ref, fetch_send.at[0], fetch_recv.at[0], WIDE - 1).wait_recv()
    left_product(me)
    for j in range(1, WIDE):
        left_product(source(0, j))

    def take(i, c):
        bulk(stage_ref, fetched_ref, fetch_send.at[0], fetch_recv.at[i], WIDE).wait_recv()
        for j in range(WIDE):
            left_product(source(i, j))
        return c

    lax.fori_loop(1, ROUNDS, take, 0)

    lane = lax.broadcasted_iota(jnp.int32, (cv, LANES), 1)

    def right_product(t, u):
        for q in range(bps):
            block = fetched_ref[slot_ref[t, q]]
            cols_ref[u, SPAN * q : SPAN * q + cv, 0:dof] = block
            cols_ref[u, SPAN * q : SPAN * q + cv, dof : 2 * dof] = block
        cols = cols_ref[u]
        one = None
        for q in range(bps - 1, -1, -1):
            prod = lax.dot_general(pk_ref[t, q], cols, NT, preferred_element_type=jnp.float32)
            one = prod if one is None else jnp.where(lane < SPAN * (q + 1), prod, one)
        code, factor = coded(one)
        code_ref[t] = code
        factor_ref[t] = as_row(factor)

    def give(i, j):
        where = target(i, j)
        peer = where[0] * 16 + where[1]
        remote(
            factor_ref.at[peer], scale_ref.at[me], fact_send.at[0], fact_recv.at[0], where
        ).start()
        remote(
            code_ref.at[peer], part_ref.at[me], part_send.at[0], part_recv.at[0], where
        ).start()

    def index(i, j):
        where = target(i, j)
        return where[0] * 16 + where[1]

    for j in range(WIDE):
        right_product(index(0, j), j)

    def work(i, c):
        for j in range(WIDE):
            right_product(index(i, j), j)

        for j in range(WIDE):
            @pl.when((i > 1) | (j > 0))
            def _():
                give(i - 1, j)
        return c

    lax.fori_loop(1, ROUNDS, work, 0)
    for j in range(WIDE):
        give(ROUNDS - 1, j)
    part_ref[me] = code_ref[me]
    scale_ref[me] = factor_ref[me]

    row_lane = lax.broadcasted_iota(jnp.int32, (1, LANES), 1)

    def locate(d, row):
        return jnp.where(row_lane == d, owner_ref[req_ref[d, 0, 0]], row)

    place = lax.fori_loop(0, n, locate, jnp.zeros((1, LANES), jnp.int32), unroll=8)
    hot = jnp.where(
        lax.broadcasted_iota(jnp.int32, (n, LANES), 0) == place, 1.0, 0.0
    ).astype(jnp.bfloat16)
    hot = jnp.concatenate([hot, hot], axis=1)

    bulk(code_ref, part_ref, part_send.at[0], part_recv.at[0], n - 1).wait()
    bulk(factor_ref, scale_ref, fact_send.at[0], fact_recv.at[0], n - 1).wait()

    blocks = [(lane + LANES * k) // cv for k in range(width // LANES)]

    def spread(d, c):
        values = part_ref[d].astype(jnp.int32).astype(jnp.float32) * as_column(scale_ref[d], cv)
        tiles = [jnp.zeros((cv, LANES), jnp.float32)] * (width // LANES)
        for q in range(bps):
            pos = req_ref[d, 0, 1 + q]
            moved = pltpu.roll(values, lax.rem(pos * cv - SPAN * q + LANES, LANES), 1)
            tiles = [jnp.where(b == pos, moved, tile) for b, tile in zip(blocks, tiles)]
        for k, tile in enumerate(tiles):
            spread_ref[k, pl.ds(d * cv, cv), :] = tile
        return c

    lax.fori_loop(0, n, spread, 0, unroll=8)

    def combine(c, carry):
        at = pl.ds(c, n, stride=cv)
        whole = jnp.concatenate(
            [spread_ref[k, at, :] for k in range(width // LANES)], axis=1
        )
        total = jnp.dot(
            hot, jnp.concatenate(split(whole), axis=0), preferred_element_type=jnp.float32
        )
        for k in range(width // LANES):
            total_ref[k, at, :] = total[:, LANES * k : LANES * (k + 1)]
        return carry

    lax.fori_loop(0, cv, combine, 0)

    def encode(o):
        rows = jnp.concatenate(
            [total_ref[k, pl.ds(o * cv, cv), :] for k in range(width // LANES)], axis=1
        )
        code, factor = coded(rows)
        rows_ref[o] = code
        rows_scale[o] = as_row(factor)

    def deliver(i, j):
        where = target(i, j)
        peer = where[0] * 16 + where[1]
        remote(
            rows_scale.at[peer], land_scale.at[me], rsc_send.at[0], rsc_recv.at[i], where
        ).start()
        remote(
            rows_ref.at[peer], land_ref.at[me], rows_send.at[0], rows_recv.at[i], where
        ).start()

    for j in range(WIDE):
        encode(index(0, j))

    def emit(i, c):
        for j in range(WIDE):
            encode(index(i, j))
        for j in range(WIDE):
            @pl.when((i > 1) | (j > 0))
            def _():
                deliver(i - 1, j)
        return c

    lax.fori_loop(1, ROUNDS, emit, 0)
    for j in range(WIDE):
        deliver(ROUNDS - 1, j)

    def out_copy(p):
        return pltpu.make_async_copy(
            wide_ref.at[p], out_ref.at[p], out_sem.at[p]
        )

    def decode(code, scale, p):
        wide_ref[p] = code.astype(jnp.int32).astype(jnp.float32) * as_column(scale, cv)

    def arrived(i, count):
        bulk(rows_ref, land_ref, rows_send.at[0], rows_recv.at[i], count).wait_recv()
        bulk(rows_scale, land_scale, rsc_send.at[0], rsc_recv.at[i], count).wait_recv()

    decode(rows_ref[me], rows_scale[me], me)
    arrived(0, WIDE - 1)
    for j in range(1, WIDE):
        p = source(0, j)
        decode(land_ref[p], land_scale[p], p)
    for j in range(WIDE):
        out_copy(source(0, j)).start()

    def drain(i, c):
        arrived(i, WIDE)
        for j in range(WIDE):
            p = source(i, j)
            decode(land_ref[p], land_scale[p], p)
        for j in range(WIDE):
            out_copy(source(i, j)).start()
        return c

    lax.fori_loop(1, ROUNDS, drain, 0)
    bulk(stage_ref, fetched_ref, fetch_send.at[0], fetch_recv.at[0], n - 1).wait_send()
    bulk(rows_ref, land_ref, rows_send.at[0], rows_recv.at[0], n - 1).wait_send()
    bulk(rows_scale, land_scale, rsc_send.at[0], rsc_recv.at[0], n - 1).wait_send()

    def finish(p, c):
        out_copy(p).wait()
        return c

    lax.fori_loop(0, n, finish, 0)


def whole(col_slot, owners, meta, prolong, stiffness):
    slots, bps, dof, _ = stiffness.shape
    cv = prolong.shape[1]
    n = meta.shape[0]
    width = MAXNB * cv
    sem = pltpu.SemaphoreType.DMA
    bf16, f32, i16, i32 = jnp.bfloat16, jnp.float32, jnp.int16, jnp.int32
    return pl.pallas_call(
        whole_kernel,
        out_shape=jax.ShapeDtypeStruct((n, cv, width), f32),
        in_specs=[SMEM, SMEM, VMEM, VMEM, HBM],
        out_specs=HBM,
        scratch_shapes=[
            pltpu.VMEM(meta.shape, i32),
            pltpu.SMEM(meta.shape, i32),
            pltpu.VMEM((n, cv, dof), bf16),
            pltpu.VMEM((n, cv, dof), bf16),
            pltpu.VMEM(stiffness.shape, bf16),
            pltpu.VMEM((n, bps, cv, 2 * dof), bf16),
            pltpu.VMEM((WIDE, LANES, 2 * dof), bf16),
            pltpu.VMEM((n, cv, LANES), i16),
            pltpu.VMEM((n, 1, LANES), f32),
            pltpu.VMEM((n, cv, LANES), i16),
            pltpu.VMEM((n, 1, LANES), f32),
            pltpu.VMEM((width // LANES, n * cv, LANES), f32),
            pltpu.VMEM((width // LANES, n * cv, LANES), f32),
            pltpu.VMEM((n, cv, width), i16),
            pltpu.VMEM((n, 1, LANES), f32),
            pltpu.VMEM((n, cv, width), i16),
            pltpu.VMEM((n, 1, LANES), f32),
            pltpu.VMEM((n, cv, width), f32),
            sem((1,)), sem((1,)),
            sem((1,)), sem((ROUNDS,)),
            sem((1,)), sem((1,)),
            sem((1,)), sem((1,)),
            sem((1,)), sem((ROUNDS,)),
            sem((1,)), sem((ROUNDS,)),
            sem((n // 16,)), sem((1,)), sem((n,)),
        ],
        compiler_params=pltpu.CompilerParams(
            collective_id=1, has_side_effects=True, vmem_limit_bytes=60 << 20
        ),
        name="whole",
    )(col_slot, owners, meta, prolong, stiffness)


def per_device(prolong, stiffness, request, col_slot, col_pos, coarse_owner):
    slots, bps = col_slot.shape
    meta = jnp.concatenate([request[:, None], col_pos], axis=1)
    meta = jnp.pad(meta, ((0, 0), (0, LANES - 1 - bps)))[:, None, :]
    return whole(col_slot, coarse_owner[:, 0], meta, prolong, stiffness)


def solution(mesh):
    placed = (
        P(AXES, None, None),
        P(AXES, None, None, None),
        P(AXES),
        P(AXES, None),
        P(AXES, None),
        P(AXES, None),
    )
    return jax.shard_map(
        per_device, mesh=mesh, in_specs=placed, out_specs=P(AXES, None, None), check_vma=False
    )
```

```python
import functools

import jax
import jax.numpy as jnp
from jax import lax
from jax.experimental import pallas as pl
from jax.experimental.pallas import tpu as pltpu
from jax.sharding import PartitionSpec as P

MAXNB = 16
AXES = ("gx", "gy")
LANES = 128
SPAN = 32
ROUNDS = 16
WIDE = 8
TOP = 32767.0
MESH = pl.DeviceIdType.MESH
HBM = pl.BlockSpec(memory_space=pl.ANY)
VMEM = pl.BlockSpec(memory_space=pltpu.VMEM)
SMEM = pl.BlockSpec(memory_space=pltpu.SMEM)
NT = (((1,), (1,)), ((), ()))


def as_row(column):
    rows = column.shape[0]
    shape = (rows, LANES)
    eye = lax.broadcasted_iota(jnp.int32, shape, 0) == lax.broadcasted_iota(jnp.int32, shape, 1)
    return jnp.sum(jnp.where(eye, column, 0.0), axis=0, keepdims=True)


def as_column(row, rows):
    shape = (rows, LANES)
    eye = lax.broadcasted_iota(jnp.int32, shape, 0) == lax.broadcasted_iota(jnp.int32, shape, 1)
    return jnp.sum(jnp.where(eye, row, 0.0), axis=1, keepdims=True)


def coded(values):
    top = jnp.maximum(jnp.max(jnp.abs(values), axis=1, keepdims=True), 1e-30)
    code = jnp.round(values * (TOP / top)).astype(jnp.int32).astype(jnp.int16)
    return code, top * (1.0 / TOP)


def split(values):
    hi = values.astype(jnp.bfloat16)
    return hi, (values - hi.astype(jnp.float32)).astype(jnp.bfloat16)


def whole_kernel(
    slot_ref, pos_ref, ask_ref, owner_ref, prolong_ref, stiff_ref,
    out_ref,
    meta_ref, mid_ref, meta_in, req_ref, stage_ref, fetched_ref, mats_ref, pk_ref, cols_ref,
    code_ref, factor_ref, part_ref, scale_ref, spread_ref, total_ref,
    rows_ref, rows_scale, land_ref, land_scale,
    near_send, near_recv, far_send, far_recv, fetch_send, fetch_recv, part_send, part_recv, fact_send, fact_recv,
    rows_send, rows_recv, rsc_send, rsc_recv, mats_sem, req_sem,
):
    n, cv, dof = fetched_ref.shape
    bps = mats_ref.shape[1]
    width = out_ref.shape[2]
    gx, gy = lax.axis_index("gx"), lax.axis_index("gy")
    me = gx * 16 + gy
    z, core = gx // 2, lax.rem(gx, 2)
    x, y = gy // 4, lax.rem(gy, 4)
    to_gx = [lax.rem(z + j // 2, 4) * 2 + lax.rem(core + j, 2) for j in range(WIDE)]
    from_gx = [lax.rem(z + 4 - j // 2, 4) * 2 + lax.rem(core + j, 2) for j in range(WIDE)]

    def target(i, j):
        s = lax.rem(i * 5 + j * 3, 16)
        return to_gx[j], lax.rem(x + s // 4, 4) * 4 + lax.rem(y + s, 4)

    def source(i, j):
        s = lax.rem(i * 5 + j * 3, 16)
        return from_gx[j] * 16 + lax.rem(x + 4 - s // 4, 4) * 4 + lax.rem(y + 16 - s, 4)

    def each(fn):
        def body(i, c):
            for j in range(WIDE):
                fn(i, j)
            return c

        for j in range(1, WIDE):
            fn(0, j)
        lax.fori_loop(1, ROUNDS, body, 0)

    def remote(src, dst, send_sem, recv_sem, where):
        return pltpu.make_async_remote_copy(
            src_ref=src, dst_ref=dst, send_sem=send_sem, recv_sem=recv_sem,
            device_id=where, device_id_type=MESH,
        )

    def bulk(src, dst, send_sem, recv_sem, count):
        return remote(
            src.at[pl.ds(0, count)], dst.at[pl.ds(0, count)], send_sem, recv_sem, (gx, gy)
        )

    loads = [
        pltpu.make_async_copy(
            stiff_ref.at[pl.ds(b * 16, 16)], mats_ref.at[pl.ds(b * 16, 16)], mats_sem.at[b]
        )
        for b in range(n // 16)
    ]
    for copy in loads:
        copy.start()

    barrier = pltpu.get_barrier_semaphore()
    near = [(g, gy) for g in to_gx[1:]]
    far = [(gx, lax.rem(x + s // 4, 4) * 4 + lax.rem(y + s, 4)) for s in range(1, 16)]
    for where in near + far:
        pl.semaphore_signal(barrier, inc=1, device_id=where, device_id_type=MESH)

    row_lane = lax.broadcasted_iota(jnp.int32, (1, LANES), 1)

    def describe(h, c):
        for g in range(8):
            p = g * 16 + h
            row = jnp.where(row_lane == 0, ask_ref[p], 0)
            for q in range(bps):
                row = jnp.where(row_lane == 1 + q, pos_ref[q, p], row)
            meta_ref[g, h] = row
        return c

    lax.fori_loop(0, 16, describe, 0)
    mid_ref[gx] = meta_ref[gx]
    cols_ref[...] = jnp.zeros_like(cols_ref)
    pl.semaphore_wait(barrier, 22)
    for where in near:
        remote(
            meta_ref.at[where[0]], mid_ref.at[gx], near_send.at[0], near_recv.at[0], where
        ).start()
    bulk(meta_ref, mid_ref, near_send.at[0], near_recv.at[0], 7).wait()
    for where in far:
        remote(
            mid_ref.at[:, where[1]], meta_in.at[:, gy], far_send.at[0], far_recv.at[0], where
        ).start()
    meta_in[:, gy] = mid_ref[:, gy]
    remote(
        mid_ref.at[:, pl.ds(0, 15)], meta_in.at[:, pl.ds(0, 15)],
        far_send.at[0], far_recv.at[0], (gx, gy),
    ).wait()
    to_scalars = pltpu.make_async_copy(meta_in, req_ref, req_sem.at[0])
    to_scalars.start()
    to_scalars.wait()

    def asked(d, k):
        return req_ref[d // 16, lax.rem(d, 16), 0, k]

    def fill(p, c):
        stage_ref[p] = prolong_ref[asked(p, 0)]
        return c

    lax.fori_loop(0, n, fill, 0, unroll=8)

    def answer(i, j):
        where = target(i, j)
        remote(
            stage_ref.at[where[0] * 16 + where[1]], fetched_ref.at[me],
            fetch_send.at[0], fetch_recv.at[i], where,
        ).start()

    each(answer)
    fetched_ref[me] = prolong_ref[asked(me, 0)]
    for copy in loads:
        copy.wait()

    def left_product(t):
        rows = fetched_ref[t]
        parts = []
        for h in range(bps // 2):
            pair = jnp.concatenate([mats_ref[t, 2 * h], mats_ref[t, 2 * h + 1]], axis=1)
            prod = jnp.dot(rows, pair, preferred_element_type=jnp.float32)
            parts += [prod[:, 0:dof], prod[:, dof : 2 * dof]]
        hi, lo = split(jnp.concatenate(parts, axis=0))
        pk_ref[t, :, 0:dof] = hi
        pk_ref[t, :, dof : 2 * dof] = lo

    bulk(stage_ref, fetched_ref, fetch_send.at[0], fetch_recv.at[0], WIDE - 1).wait_recv()
    left_product(me)
    for j in range(1, WIDE):
        left_product(source(0, j))

    def take(i, c):
        bulk(stage_ref, fetched_ref, fetch_send.at[0], fetch_recv.at[i], WIDE).wait_recv()
        for j in range(WIDE):
            left_product(source(i, j))
        return c

    lax.fori_loop(1, ROUNDS, take, 0)

    lane = lax.broadcasted_iota(jnp.int32, (cv, LANES), 1)

    def right_product(t, u):
        for q in range(bps):
            block = fetched_ref[slot_ref[q, t]]
            cols_ref[u, SPAN * q : SPAN * q + cv, 0:dof] = block
            cols_ref[u, SPAN * q : SPAN * q + cv, dof : 2 * dof] = block
        prod = lax.dot_general(pk_ref[t], cols_ref[u], NT, preferred_element_type=jnp.float32)
        one = prod[(bps - 1) * cv :]
        for q in range(bps - 2, -1, -1):
            one = jnp.where(lane < SPAN * (q + 1), prod[q * cv : (q + 1) * cv], one)
        code, factor = coded(one)
        code_ref[t] = code
        factor_ref[t] = as_row(factor)

    def give(i, j):
        where = target(i, j)
        peer = where[0] * 16 + where[1]
        remote(
            factor_ref.at[peer], scale_ref.at[me], fact_send.at[0], fact_recv.at[0], where
        ).start()
        remote(
            code_ref.at[peer], part_ref.at[me], part_send.at[0], part_recv.at[0], where
        ).start()

    def index(i, j):
        where = target(i, j)
        return where[0] * 16 + where[1]

    for j in range(WIDE):
        right_product(index(0, j), j)

    def work(i, c):
        for j in range(WIDE):
            right_product(index(i, j), j)

        for j in range(WIDE):
            @pl.when((i > 1) | (j > 0))
            def _():
                give(i - 1, j)
        return c

    lax.fori_loop(1, ROUNDS, work, 0)
    for j in range(WIDE):
        give(ROUNDS - 1, j)
    part_ref[me] = code_ref[me]
    scale_ref[me] = factor_ref[me]

    def locate(d, row):
        return jnp.where(row_lane == d, owner_ref[asked(d, 0)], row)

    place = lax.fori_loop(0, n, locate, jnp.zeros((1, LANES), jnp.int32), unroll=8)
    hot = jnp.where(
        lax.broadcasted_iota(jnp.int32, (n, LANES), 0) == place, 1.0, 0.0
    ).astype(jnp.bfloat16)
    hot = jnp.concatenate([hot, hot], axis=1)

    bulk(code_ref, part_ref, part_send.at[0], part_recv.at[0], n - 1).wait()
    bulk(factor_ref, scale_ref, fact_send.at[0], fact_recv.at[0], n - 1).wait()

    blocks = [(lane + LANES * k) // cv for k in range(width // LANES)]

    def spread(d, c):
        values = part_ref[d].astype(jnp.int32).astype(jnp.float32) * as_column(scale_ref[d], cv)
        tiles = [jnp.zeros((cv, LANES), jnp.float32)] * (width // LANES)
        for q in range(bps):
            pos = asked(d, 1 + q)
            moved = pltpu.roll(values, lax.rem(pos * cv - SPAN * q + LANES, LANES), 1)
            tiles = [jnp.where(b == pos, moved, tile) for b, tile in zip(blocks, tiles)]
        for k, tile in enumerate(tiles):
            spread_ref[k, pl.ds(d * cv, cv), :] = tile
        return c

    lax.fori_loop(0, n, spread, 0, unroll=8)

    def combine(c, carry):
        at = pl.ds(c, n, stride=cv)
        whole = jnp.concatenate(
            [spread_ref[k, at, :] for k in range(width // LANES)], axis=1
        )
        total = jnp.dot(
            hot, jnp.concatenate(split(whole), axis=0), preferred_element_type=jnp.float32
        )
        for k in range(width // LANES):
            total_ref[k, at, :] = total[:, LANES * k : LANES * (k + 1)]
        return carry

    lax.fori_loop(0, cv, combine, 0)

    def encode(o):
        rows = jnp.concatenate(
            [total_ref[k, pl.ds(o * cv, cv), :] for k in range(width // LANES)], axis=1
        )
        code, factor = coded(rows)
        rows_ref[o] = code
        rows_scale[o] = as_row(factor)

    def deliver(i, j):
        where = target(i, j)
        peer = where[0] * 16 + where[1]
        remote(
            rows_scale.at[peer], land_scale.at[me], rsc_send.at[0], rsc_recv.at[i], where
        ).start()
        remote(
            rows_ref.at[peer], land_ref.at[me], rows_send.at[0], rows_recv.at[i], where
        ).start()

    for j in range(WIDE):
        encode(index(0, j))

    def emit(i, c):
        for j in range(WIDE):
            encode(index(i, j))
        for j in range(WIDE):
            @pl.when((i > 1) | (j > 0))
            def _():
                deliver(i - 1, j)
        return c

    lax.fori_loop(1, ROUNDS, emit, 0)
    for j in range(WIDE):
        deliver(ROUNDS - 1, j)

    def decode(code, scale, p):
        out_ref[p] = code.astype(jnp.int32).astype(jnp.float32) * as_column(scale, cv)

    def arrived(i, count):
        bulk(rows_ref, land_ref, rows_send.at[0], rows_recv.at[i], count).wait_recv()
        bulk(rows_scale, land_scale, rsc_send.at[0], rsc_recv.at[i], count).wait_recv()

    decode(rows_ref[me], rows_scale[me], me)
    arrived(0, WIDE - 1)
    for j in range(1, WIDE):
        p = source(0, j)
        decode(land_ref[p], land_scale[p], p)

    def drain(i, c):
        arrived(i, WIDE)
        for j in range(WIDE):
            p = source(i, j)
            decode(land_ref[p], land_scale[p], p)
        return c

    lax.fori_loop(1, ROUNDS, drain, 0)
    bulk(stage_ref, fetched_ref, fetch_send.at[0], fetch_recv.at[0], n - 1).wait_send()
    bulk(rows_ref, land_ref, rows_send.at[0], rows_recv.at[0], n - 1).wait_send()
    bulk(rows_scale, land_scale, rsc_send.at[0], rsc_recv.at[0], n - 1).wait_send()


def whole(col_slot, col_pos, request, owners, prolong, stiffness):
    slots, bps, dof, _ = stiffness.shape
    cv = prolong.shape[1]
    n = slots
    width = MAXNB * cv
    sem = pltpu.SemaphoreType.DMA
    bf16, f32, i16, i32 = jnp.bfloat16, jnp.float32, jnp.int16, jnp.int32
    return pl.pallas_call(
        whole_kernel,
        out_shape=jax.ShapeDtypeStruct((n, cv, width), f32),
        in_specs=[SMEM, SMEM, SMEM, SMEM, VMEM, HBM],
        out_specs=VMEM,
        scratch_shapes=[
            pltpu.VMEM((8, 16, 1, LANES), i32),
            pltpu.VMEM((8, 16, 1, LANES), i32),
            pltpu.VMEM((8, 16, 1, LANES), i32),
            pltpu.SMEM((8, 16, 1, LANES), i32),
            pltpu.VMEM((n, cv, dof), bf16),
            pltpu.VMEM((n, cv, dof), bf16),
            pltpu.VMEM(stiffness.shape, bf16),
            pltpu.VMEM((n, bps * cv, 2 * dof), bf16),
            pltpu.VMEM((WIDE, LANES, 2 * dof), bf16),
            pltpu.VMEM((n, cv, LANES), i16),
            pltpu.VMEM((n, 1, LANES), f32),
            pltpu.VMEM((n, cv, LANES), i16),
            pltpu.VMEM((n, 1, LANES), f32),
            pltpu.VMEM((width // LANES, n * cv, LANES), f32),
            pltpu.VMEM((width // LANES, n * cv, LANES), f32),
            pltpu.VMEM((n, cv, width), i16),
            pltpu.VMEM((n, 1, LANES), f32),
            pltpu.VMEM((n, cv, width), i16),
            pltpu.VMEM((n, 1, LANES), f32),
            sem((1,)), sem((1,)),
            sem((1,)), sem((1,)),
            sem((1,)), sem((ROUNDS,)),
            sem((1,)), sem((1,)),
            sem((1,)), sem((1,)),
            sem((1,)), sem((ROUNDS,)),
            sem((1,)), sem((ROUNDS,)),
            sem((n // 16,)), sem((1,)),
        ],
        compiler_params=pltpu.CompilerParams(
            collective_id=1, has_side_effects=True, vmem_limit_bytes=50 << 20
        ),
        name="whole",
    )(col_slot, col_pos, request, owners, prolong, stiffness)


def per_device(prolong, stiffness, request, col_slot, col_pos, coarse_owner):
    return whole(col_slot.T, col_pos.T, request, coarse_owner[:, 0], prolong, stiffness)


def solution(mesh):
    placed = (
        P(AXES, None, None),
        P(AXES, None, None, None),
        P(AXES),
        P(AXES, None),
        P(AXES, None),
        P(AXES, None),
    )
    return jax.shard_map(
        per_device, mesh=mesh, in_specs=placed, out_specs=P(AXES, None, None), check_vma=False
    )
```

```python
import functools

import jax
import jax.numpy as jnp
from jax import lax
from jax.experimental import pallas as pl
from jax.experimental.pallas import tpu as pltpu
from jax.sharding import PartitionSpec as P

MAXNB = 16
AXES = ("gx", "gy")
LANES = 128
SPAN = 32
CHUNKS = ((0, 8), (8, 16))
ROUNDS = 16
WIDE = 8
TOP = 32767.0
MESH = pl.DeviceIdType.MESH
HBM = pl.BlockSpec(memory_space=pltpu.HBM)
VMEM = pl.BlockSpec(memory_space=pltpu.VMEM)
NT = (((1,), (1,)), ((), ()))


def diagonal(rows, first):
    shape = (rows, LANES)
    return (
        lax.broadcasted_iota(jnp.int32, shape, 0) + first
        == lax.broadcasted_iota(jnp.int32, shape, 1)
    )


def as_row(column, first=0):
    return jnp.sum(
        jnp.where(diagonal(column.shape[0], first), column, 0.0), axis=0, keepdims=True
    )


def as_column(row, rows, first=0):
    return jnp.sum(jnp.where(diagonal(rows, first), row, 0.0), axis=1, keepdims=True)


def coded(values):
    top = jnp.maximum(jnp.max(jnp.abs(values), axis=1, keepdims=True), 1e-30)
    code = jnp.round(values * (TOP / top)).astype(jnp.int32)
    return code, top * (1.0 / TOP)


def split(values):
    hi = values.astype(jnp.bfloat16)
    return hi, (values - hi.astype(jnp.float32)).astype(jnp.bfloat16)


def whole_kernel(
    slot_in, pos_in, ask_in, owner_in, prolong_in, stiff_ref,
    out_ref,
    slot_ref, pos_ref, ask_ref, owner_ref, prolong_ref,
    meta_ref, mid_ref, meta_in, req_ref, stage_ref, fetched_ref, mats_ref, pk_ref, cols_ref,
    code_a, code_b, factor_ref, part_a, part_b, scale_ref, table_ref, spread_ref, total_ref,
    rows_a, rows_b, rows_scale, land_a, land_b, land_scale,
    near_send, near_recv, far_send, far_recv, fetch_send, fetch_recv, part_send, part_recv, fact_send, fact_recv,
    rows_send, rows_recv, rsc_send, rsc_recv, mats_sem, req_sem, arg_sem,
):
    n, cv, dof = fetched_ref.shape
    bps = mats_ref.shape[1]
    width = out_ref.shape[2]
    gx, gy = lax.axis_index("gx"), lax.axis_index("gy")
    me = gx * 16 + gy
    z, core = gx // 2, lax.rem(gx, 2)
    x, y = gy // 4, lax.rem(gy, 4)
    to_gx = [lax.rem(z + j // 2, 4) * 2 + lax.rem(core + j, 2) for j in range(WIDE)]
    from_gx = [lax.rem(z + 4 - j // 2, 4) * 2 + lax.rem(core + j, 2) for j in range(WIDE)]

    def target(i, j):
        s = lax.rem(i * 5 + j * 3, 16)
        return to_gx[j], lax.rem(x + s // 4, 4) * 4 + lax.rem(y + s, 4)

    def source(i, j):
        s = lax.rem(i * 5 + j * 3, 16)
        return from_gx[j] * 16 + lax.rem(x + 4 - s // 4, 4) * 4 + lax.rem(y + 16 - s, 4)

    def each(fn):
        def body(i, c):
            for j in range(WIDE):
                fn(i, j)
            return c

        for j in range(1, WIDE):
            fn(0, j)
        lax.fori_loop(1, ROUNDS, body, 0)

    def remote(src, dst, send_sem, recv_sem, where):
        return pltpu.make_async_remote_copy(
            src_ref=src, dst_ref=dst, send_sem=send_sem, recv_sem=recv_sem,
            device_id=where, device_id_type=MESH,
        )

    def bulk(src, dst, send_sem, recv_sem, count):
        return remote(
            src.at[pl.ds(0, count)], dst.at[pl.ds(0, count)], send_sem, recv_sem, (gx, gy)
        )

    small = [
        pltpu.make_async_copy(src, dst, arg_sem.at[k])
        for k, (src, dst) in enumerate(
            (
                (ask_in, ask_ref), (pos_in, pos_ref), (slot_in, slot_ref),
                (owner_in, owner_ref), (prolong_in, prolong_ref),
            )
        )
    ]
    for copy in small:
        copy.start()
    loads = [
        pltpu.make_async_copy(
            stiff_ref.at[pl.ds(b * 16, 16)], mats_ref.at[pl.ds(b * 16, 16)], mats_sem.at[b]
        )
        for b in range(n // 16)
    ]
    for copy in loads:
        copy.start()

    barrier = pltpu.get_barrier_semaphore()
    near = [(g, gy) for g in to_gx[1:]]
    far = [(gx, lax.rem(x + s // 4, 4) * 4 + lax.rem(y + s, 4)) for s in range(1, 16)]
    for where in near + far:
        pl.semaphore_signal(barrier, inc=1, device_id=where, device_id_type=MESH)

    row_lane = lax.broadcasted_iota(jnp.int32, (1, LANES), 1)

    def describe(h, c):
        for g in range(8):
            p = g * 16 + h
            row = jnp.where(row_lane == 0, ask_ref[p], 0)
            for q in range(bps):
                row = jnp.where(row_lane == 1 + q, pos_ref[q, p], row)
            meta_ref[g, h] = row
        return c

    for copy in small[:2]:
        copy.wait()
    lax.fori_loop(0, 16, describe, 0)
    mid_ref[gx] = meta_ref[gx]
    cols_ref[...] = jnp.zeros_like(cols_ref)
    unit_row = lax.broadcasted_iota(jnp.int32, (SPAN, width), 0)
    unit_col = lax.broadcasted_iota(jnp.int32, (SPAN, width), 1)
    for k in range(MAXNB):
        unit = (unit_row < cv) & (unit_col == unit_row + cv * k)
        table_ref[k] = jnp.where(unit, 1.0, 0.0).astype(jnp.bfloat16)
    pl.semaphore_wait(barrier, 22)
    for where in near:
        remote(
            meta_ref.at[where[0]], mid_ref.at[gx], near_send.at[0], near_recv.at[0], where
        ).start()
    bulk(meta_ref, mid_ref, near_send.at[0], near_recv.at[0], 7).wait()
    for where in far:
        remote(
            mid_ref.at[:, where[1]], meta_in.at[:, gy], far_send.at[0], far_recv.at[0], where
        ).start()
    meta_in[:, gy] = mid_ref[:, gy]
    remote(
        mid_ref.at[:, pl.ds(0, 15)], meta_in.at[:, pl.ds(0, 15)],
        far_send.at[0], far_recv.at[0], (gx, gy),
    ).wait()
    for copy in small[2:]:
        copy.wait()
    to_scalars = pltpu.make_async_copy(meta_in, req_ref, req_sem.at[0])
    to_scalars.start()
    to_scalars.wait()

    def asked(d, k):
        return req_ref[d // 16, lax.rem(d, 16), 0, k]

    def fill(p, c):
        stage_ref[p] = prolong_ref[asked(p, 0)]
        return c

    lax.fori_loop(0, n, fill, 0, unroll=8)

    def answer(i, j):
        where = target(i, j)
        remote(
            stage_ref.at[where[0] * 16 + where[1]], fetched_ref.at[me],
            fetch_send.at[0], fetch_recv.at[i], where,
        ).start()

    each(answer)
    fetched_ref[me] = prolong_ref[asked(me, 0)]
    for copy in loads:
        copy.wait()

    def left_product(t):
        rows = fetched_ref[t]
        parts = []
        for h in range(bps // 2):
            pair = jnp.concatenate([mats_ref[t, 2 * h], mats_ref[t, 2 * h + 1]], axis=1)
            prod = jnp.dot(rows, pair, preferred_element_type=jnp.float32)
            parts += [prod[:, 0:dof], prod[:, dof : 2 * dof]]
        hi, lo = split(jnp.concatenate(parts, axis=0))
        pk_ref[t, :, 0:dof] = hi
        pk_ref[t, :, dof : 2 * dof] = lo

    bulk(stage_ref, fetched_ref, fetch_send.at[0], fetch_recv.at[0], WIDE - 1).wait_recv()
    left_product(me)
    for j in range(1, WIDE):
        left_product(source(0, j))

    def take(i, c):
        bulk(stage_ref, fetched_ref, fetch_send.at[0], fetch_recv.at[i], WIDE).wait_recv()
        for j in range(WIDE):
            left_product(source(i, j))
        return c

    lax.fori_loop(1, ROUNDS, take, 0)

    lane = lax.broadcasted_iota(jnp.int32, (cv, LANES), 1)

    def right_product(t, u):
        for q in range(bps):
            block = fetched_ref[slot_ref[q, t]]
            cols_ref[u, SPAN * q : SPAN * q + cv, 0:dof] = block
            cols_ref[u, SPAN * q : SPAN * q + cv, dof : 2 * dof] = block
        prod = lax.dot_general(pk_ref[t], cols_ref[u], NT, preferred_element_type=jnp.float32)
        one = prod[(bps - 1) * cv :]
        for q in range(bps - 2, -1, -1):
            one = jnp.where(lane < SPAN * (q + 1), prod[q * cv : (q + 1) * cv], one)
        code, factor = coded(one)
        for (first, rows), ref in zip(CHUNKS, (code_a, code_b)):
            ref[t] = code[first : first + rows].astype(jnp.int16)
        factor_ref[t] = as_row(factor)

    def give(i, j):
        where = target(i, j)
        peer = where[0] * 16 + where[1]
        remote(
            factor_ref.at[peer], scale_ref.at[me], fact_send.at[0], fact_recv.at[0], where
        ).start()
        remote(
            code_a.at[peer], part_a.at[me], part_send.at[0], part_recv.at[0], where
        ).start()

    def give_rest(i, j):
        where = target(i, j)
        remote(
            code_b.at[where[0] * 16 + where[1]], part_b.at[me],
            part_send.at[1], part_recv.at[1], where,
        ).start()

    def index(i, j):
        where = target(i, j)
        return where[0] * 16 + where[1]

    for j in range(WIDE):
        right_product(index(0, j), j)

    def work(i, c):
        for j in range(WIDE):
            right_product(index(i, j), j)

        for j in range(WIDE):
            @pl.when((i > 1) | (j > 0))
            def _():
                give(i - 1, j)
        return c

    lax.fori_loop(1, ROUNDS, work, 0)
    for j in range(WIDE):
        give(ROUNDS - 1, j)
    each(give_rest)
    part_a[me] = code_a[me]
    part_b[me] = code_b[me]
    scale_ref[me] = factor_ref[me]

    def locate(d, row):
        return jnp.where(row_lane == d, owner_ref[asked(d, 0)], row)

    place = lax.fori_loop(0, n, locate, jnp.zeros((1, LANES), jnp.int32), unroll=8)
    hot = jnp.where(
        lax.broadcasted_iota(jnp.int32, (n, LANES), 0) == place, 1.0, 0.0
    ).astype(jnp.bfloat16)
    hot = jnp.concatenate([hot, hot], axis=1)

    tiles = width // LANES

    def spread(part, first, rows, d):
        values = part[d].astype(jnp.int32).astype(jnp.float32)
        values = values * as_column(scale_ref[d], rows, first)
        hi = values.astype(jnp.bfloat16).astype(jnp.float32)
        both = jnp.concatenate([hi, values - hi], axis=0).astype(jnp.bfloat16)
        units = jnp.concatenate(
            [table_ref[asked(d, 1 + q)] for q in range(bps)], axis=0
        )
        moved = jnp.dot(both, units, preferred_element_type=jnp.float32)
        moved = moved[:rows] + moved[rows:]
        for k in range(tiles):
            spread_ref[k, pl.ds(d * cv + first, rows), :] = moved[:, LANES * k : LANES * (k + 1)]

    def combine(c, carry):
        at = pl.ds(c, n, stride=cv)
        every = jnp.concatenate([spread_ref[k, at, :] for k in range(tiles)], axis=1)
        total = jnp.dot(
            hot, jnp.concatenate(split(every), axis=0), preferred_element_type=jnp.float32
        )
        for k in range(tiles):
            total_ref[k, at, :] = total[:, LANES * k : LANES * (k + 1)]
        return carry

    for h, ((first, rows), code_ref, part, rows_ref, land_ref) in enumerate(
        zip(CHUNKS, (code_a, code_b), (part_a, part_b), (rows_a, rows_b), (land_a, land_b))
    ):
        bulk(code_ref, part, part_send.at[h], part_recv.at[h], n - 1).wait()
        if h == 0:
            bulk(factor_ref, scale_ref, fact_send.at[0], fact_recv.at[0], n - 1).wait()

        def spread_some(i, c):
            for j in range(WIDE):
                spread(part, first, rows, i * WIDE + j)
            return c

        lax.fori_loop(0, ROUNDS, spread_some, 0)
        lax.fori_loop(first, first + rows, combine, 0)

        def encode(o):
            row = jnp.concatenate(
                [total_ref[k, pl.ds(o * cv + first, rows), :] for k in range(tiles)], axis=1
            )
            code, factor = coded(row)
            rows_ref[o] = code.astype(jnp.int16)
            rows_scale[h, o] = as_row(factor, first)

        def deliver(i, j):
            where = target(i, j)
            peer = where[0] * 16 + where[1]
            remote(
                rows_scale.at[h, peer], land_scale.at[h, me],
                rsc_send.at[h], rsc_recv.at[h, i], where,
            ).start()
            remote(
                rows_ref.at[peer], land_ref.at[me],
                rows_send.at[h], rows_recv.at[h, i], where,
            ).start()

        for j in range(WIDE):
            encode(index(0, j))

        def emit(i, c):
            for j in range(WIDE):
                encode(index(i, j))
            for j in range(WIDE):
                @pl.when((i > 1) | (j > 0))
                def _():
                    deliver(i - 1, j)
            return c

        lax.fori_loop(1, ROUNDS, emit, 0)
        for j in range(WIDE):
            deliver(ROUNDS - 1, j)

    for h, ((first, rows), rows_ref, land_ref) in enumerate(
        zip(CHUNKS, (rows_a, rows_b), (land_a, land_b))
    ):
        def decode(code, scale, p):
            out_ref[p, first : first + rows, :] = code.astype(jnp.int32).astype(
                jnp.float32
            ) * as_column(scale, rows, first)

        def arrived(i, count):
            bulk(rows_ref, land_ref, rows_send.at[h], rows_recv.at[h, i], count).wait_recv()
            bulk(
                rows_scale.at[h], land_scale.at[h], rsc_send.at[h], rsc_recv.at[h, i], count
            ).wait_recv()

        decode(rows_ref[me], rows_scale[h, me], me)
        arrived(0, WIDE - 1)
        for j in range(1, WIDE):
            p = source(0, j)
            decode(land_ref[p], land_scale[h, p], p)

        def drain(i, c):
            arrived(i, WIDE)
            for j in range(WIDE):
                p = source(i, j)
                decode(land_ref[p], land_scale[h, p], p)
            return c

        lax.fori_loop(1, ROUNDS, drain, 0)
        bulk(rows_ref, land_ref, rows_send.at[h], rows_recv.at[h, 0], n - 1).wait_send()
        bulk(
            rows_scale.at[h], land_scale.at[h], rsc_send.at[h], rsc_recv.at[h, 0], n - 1
        ).wait_send()
    bulk(stage_ref, fetched_ref, fetch_send.at[0], fetch_recv.at[0], n - 1).wait_send()


def whole(col_slot, col_pos, request, owners, prolong, stiffness):
    slots, bps, dof, _ = stiffness.shape
    cv = prolong.shape[1]
    n = slots
    width = MAXNB * cv
    sem = pltpu.SemaphoreType.DMA
    bf16, f32, i16, i32 = jnp.bfloat16, jnp.float32, jnp.int16, jnp.int32
    return pl.pallas_call(
        whole_kernel,
        out_shape=jax.ShapeDtypeStruct((n, cv, width), f32),
        in_specs=[HBM] * 6,
        out_specs=VMEM,
        scratch_shapes=[
            pltpu.SMEM(col_slot.shape, i32),
            pltpu.SMEM(col_pos.shape, i32),
            pltpu.SMEM(request.shape, i32),
            pltpu.SMEM(owners.shape, i32),
            pltpu.VMEM(prolong.shape, bf16),
            pltpu.VMEM((8, 16, 1, LANES), i32),
            pltpu.VMEM((8, 16, 1, LANES), i32),
            pltpu.VMEM((8, 16, 1, LANES), i32),
            pltpu.SMEM((8, 16, 1, LANES), i32),
            pltpu.VMEM((n, cv, dof), bf16),
            pltpu.VMEM((n, cv, dof), bf16),
            pltpu.VMEM(stiffness.shape, bf16),
            pltpu.VMEM((n, bps * cv, 2 * dof), bf16),
            pltpu.VMEM((WIDE, LANES, 2 * dof), bf16),
            *[pltpu.VMEM((n, rows, LANES), i16) for _, rows in CHUNKS],
            pltpu.VMEM((n, 1, LANES), f32),
            *[pltpu.VMEM((n, rows, LANES), i16) for _, rows in CHUNKS],
            pltpu.VMEM((n, 1, LANES), f32),
            pltpu.VMEM((MAXNB, SPAN, width), bf16),
            pltpu.VMEM((width // LANES, n * cv, LANES), f32),
            pltpu.VMEM((width // LANES, n * cv, LANES), f32),
            *[pltpu.VMEM((n, rows, width), i16) for _, rows in CHUNKS],
            pltpu.VMEM((len(CHUNKS), n, 1, LANES), f32),
            *[pltpu.VMEM((n, rows, width), i16) for _, rows in CHUNKS],
            pltpu.VMEM((len(CHUNKS), n, 1, LANES), f32),
            sem((1,)), sem((1,)),
            sem((1,)), sem((1,)),
            sem((1,)), sem((ROUNDS,)),
            sem((2,)), sem((2,)),
            sem((1,)), sem((1,)),
            sem((2,)), sem((2, ROUNDS)),
            sem((2,)), sem((2, ROUNDS)),
            sem((n // 16,)), sem((1,)), sem((5,)),
        ],
        compiler_params=pltpu.CompilerParams(
            collective_id=1, has_side_effects=True, vmem_limit_bytes=44 << 20
        ),
        name="whole",
    )(col_slot, col_pos, request, owners, prolong, stiffness)


def per_device(prolong, stiffness, request, col_slot, col_pos, coarse_owner):
    return whole(col_slot.T, col_pos.T, request, coarse_owner[:, 0], prolong, stiffness)


def solution(mesh):
    placed = (
        P(AXES, None, None),
        P(AXES, None, None, None),
        P(AXES),
        P(AXES, None),
        P(AXES, None),
        P(AXES, None),
    )
    return jax.shard_map(
        per_device, mesh=mesh, in_specs=placed, out_specs=P(AXES, None, None), check_vma=False
    )
```

```python
import functools

import jax
import jax.numpy as jnp
from jax import lax
from jax.experimental import pallas as pl
from jax.experimental.pallas import tpu as pltpu
from jax.sharding import PartitionSpec as P

MAXNB = 16
AXES = ("gx", "gy")
LANES = 128
SPAN = 32
PITCH = 28
CHUNKS = ((0, 8), (8, 16))
ROUNDS = 16
WIDE = 8
TOP = 32767.0
MESH = pl.DeviceIdType.MESH
HBM = pl.BlockSpec(memory_space=pltpu.HBM)
VMEM = pl.BlockSpec(memory_space=pltpu.VMEM)
NT = (((1,), (1,)), ((), ()))


def diagonal(rows, first):
    shape = (rows, LANES)
    return (
        lax.broadcasted_iota(jnp.int32, shape, 0) + first
        == lax.broadcasted_iota(jnp.int32, shape, 1)
    )


def as_row(column, first=0):
    return jnp.sum(
        jnp.where(diagonal(column.shape[0], first), column, 0.0), axis=0, keepdims=True
    )


def as_column(row, rows, first=0):
    return jnp.sum(jnp.where(diagonal(rows, first), row, 0.0), axis=1, keepdims=True)


def coded(values):
    top = jnp.maximum(jnp.max(jnp.abs(values), axis=1, keepdims=True), 1e-30)
    code = jnp.round(values * (TOP / top)).astype(jnp.int32)
    return code, top * (1.0 / TOP)


def split(values):
    hi = values.astype(jnp.bfloat16)
    return hi, (values - hi.astype(jnp.float32)).astype(jnp.bfloat16)


def whole_kernel(
    slot_in, pos_in, ask_in, owner_in, prolong_in, stiff_ref,
    out_ref,
    slot_ref, pos_ref, ask_ref, owner_ref, prolong_ref,
    meta_ref, mid_ref, req_ref, stage_ref, fetched_ref, mats_ref, pk_ref, cols_ref,
    code_a, code_b, factor_ref, part_a, part_b, scale_ref, table_ref, spread_ref, total_ref,
    rows_a, rows_b, rows_scale, land_a, land_b, land_scale,
    near_send, near_recv, far_send, far_recv, fetch_send, fetch_recv, part_send, part_recv, fact_send, fact_recv,
    rows_send, rows_recv, rsc_send, rsc_recv, mats_sem, req_sem, arg_sem,
):
    n, cv, dof = fetched_ref.shape
    bps = mats_ref.shape[1]
    width = out_ref.shape[2]
    gx, gy = lax.axis_index("gx"), lax.axis_index("gy")
    me = gx * 16 + gy
    z, core = gx // 2, lax.rem(gx, 2)
    x, y = gy // 4, lax.rem(gy, 4)
    to_gx = [lax.rem(z + j // 2, 4) * 2 + lax.rem(core + j, 2) for j in range(WIDE)]
    from_gx = [lax.rem(z + 4 - j // 2, 4) * 2 + lax.rem(core + j, 2) for j in range(WIDE)]

    def target(i, j):
        s = lax.rem(i * 5 + j * 3, 16)
        return to_gx[j], lax.rem(x + s // 4, 4) * 4 + lax.rem(y + s, 4)

    def source(i, j):
        s = lax.rem(i * 5 + j * 3, 16)
        return from_gx[j] * 16 + lax.rem(x + 4 - s // 4, 4) * 4 + lax.rem(y + 16 - s, 4)

    def each(fn):
        def body(i, c):
            for j in range(WIDE):
                fn(i, j)
            return c

        for j in range(1, WIDE):
            fn(0, j)
        lax.fori_loop(1, ROUNDS, body, 0)

    def remote(src, dst, send_sem, recv_sem, where):
        return pltpu.make_async_remote_copy(
            src_ref=src, dst_ref=dst, send_sem=send_sem, recv_sem=recv_sem,
            device_id=where, device_id_type=MESH,
        )

    def bulk(src, dst, send_sem, recv_sem, count):
        return remote(
            src.at[pl.ds(0, count)], dst.at[pl.ds(0, count)], send_sem, recv_sem, (gx, gy)
        )

    small = [
        pltpu.make_async_copy(src, dst, arg_sem.at[k])
        for k, (src, dst) in enumerate(
            (
                (ask_in, ask_ref), (pos_in, pos_ref), (slot_in, slot_ref),
                (owner_in, owner_ref), (prolong_in, prolong_ref),
            )
        )
    ]
    for copy in small:
        copy.start()
    loads = [
        pltpu.make_async_copy(
            stiff_ref.at[pl.ds(b * 16, 16)], mats_ref.at[pl.ds(b * 16, 16)], mats_sem.at[b]
        )
        for b in range(n // 16)
    ]
    for copy in loads:
        copy.start()

    barrier = pltpu.get_barrier_semaphore()
    near = [(g, gy) for g in to_gx[1:]]
    far = [(gx, lax.rem(x + s // 4, 4) * 4 + lax.rem(y + s, 4)) for s in range(1, 16)]
    for where in near + far:
        pl.semaphore_signal(barrier, inc=1, device_id=where, device_id_type=MESH)

    row_lane = lax.broadcasted_iota(jnp.int32, (1, LANES), 1)

    def describe(h, c):
        for g in range(8):
            p = g * 16 + h
            row = jnp.where(row_lane == 0, ask_ref[p], 0)
            for q in range(bps):
                row = jnp.where(row_lane == 1 + q, pos_ref[q, p], row)
            meta_ref[g, h] = row
        return c

    for copy in small[:2]:
        copy.wait()
    lax.fori_loop(0, 16, describe, 0)
    mid_ref[gx] = meta_ref[gx]
    cols_ref[...] = jnp.zeros_like(cols_ref)
    unit_row = lax.broadcasted_iota(jnp.int32, (SPAN, width), 0)
    unit_col = lax.broadcasted_iota(jnp.int32, (SPAN, width), 1)
    for k in range(MAXNB):
        unit = (unit_row < cv) & (unit_col == unit_row + cv * k)
        table_ref[k] = jnp.where(unit, 1.0, 0.0).astype(jnp.bfloat16)
    pl.semaphore_wait(barrier, 22)
    for where in near:
        remote(
            meta_ref.at[where[0]], mid_ref.at[gx], near_send.at[0], near_recv.at[0], where
        ).start()
    bulk(meta_ref, mid_ref, near_send.at[0], near_recv.at[0], 7).wait()
    for where in far:
        remote(
            mid_ref.at[:, where[1]], req_ref.at[:, gy], far_send.at[0], far_recv.at[0], where
        ).start()
    to_scalars = pltpu.make_async_copy(mid_ref.at[:, gy], req_ref.at[:, gy], req_sem.at[0])
    to_scalars.start()
    remote(
        mid_ref.at[:, pl.ds(0, 15)], req_ref.at[:, pl.ds(0, 15)],
        far_send.at[0], far_recv.at[0], (gx, gy),
    ).wait()
    for copy in small[2:]:
        copy.wait()
    to_scalars.wait()

    def asked(d, k):
        return req_ref[d // 16, lax.rem(d, 16), 0, k]

    def fill(p, c):
        stage_ref[p] = prolong_ref[asked(p, 0)]
        return c

    lax.fori_loop(0, n, fill, 0, unroll=8)

    def answer(i, j):
        where = target(i, j)
        remote(
            stage_ref.at[where[0] * 16 + where[1]], fetched_ref.at[me],
            fetch_send.at[0], fetch_recv.at[i], where,
        ).start()

    each(answer)
    fetched_ref[me] = prolong_ref[asked(me, 0)]
    for copy in loads:
        copy.wait()

    def left_product(t):
        rows = fetched_ref[t]
        parts = []
        for h in range(bps // 2):
            pair = jnp.concatenate([mats_ref[t, 2 * h], mats_ref[t, 2 * h + 1]], axis=1)
            prod = jnp.dot(rows, pair, preferred_element_type=jnp.float32)
            parts += [prod[:, 0:dof], prod[:, dof : 2 * dof]]
        hi, lo = split(jnp.concatenate(parts, axis=0))
        pk_ref[t, :, 0:dof] = hi
        pk_ref[t, :, dof : 2 * dof] = lo

    bulk(stage_ref, fetched_ref, fetch_send.at[0], fetch_recv.at[0], WIDE - 1).wait_recv()
    left_product(me)
    for j in range(1, WIDE):
        left_product(source(0, j))

    def take(i, c):
        bulk(stage_ref, fetched_ref, fetch_send.at[0], fetch_recv.at[i], WIDE).wait_recv()
        for j in range(WIDE):
            left_product(source(i, j))
        return c

    lax.fori_loop(1, ROUNDS, take, 0)

    lane = lax.broadcasted_iota(jnp.int32, (cv, LANES), 1)

    def right_product(t, u):
        for q in range(bps):
            block = fetched_ref[slot_ref[q, t]]
            cols_ref[u, SPAN * q : SPAN * q + cv, 0:dof] = block
            cols_ref[u, SPAN * q : SPAN * q + cv, dof : 2 * dof] = block
        prod = lax.dot_general(pk_ref[t], cols_ref[u], NT, preferred_element_type=jnp.float32)
        one = prod[(bps - 1) * cv :]
        for q in range(bps - 2, -1, -1):
            one = jnp.where(lane < SPAN * (q + 1), prod[q * cv : (q + 1) * cv], one)
        code, factor = coded(one)
        for (first, rows), ref in zip(CHUNKS, (code_a, code_b)):
            ref[t] = code[first : first + rows].astype(jnp.int16)
        factor_ref[t] = as_row(factor)

    def give(i, j):
        where = target(i, j)
        peer = where[0] * 16 + where[1]
        remote(
            factor_ref.at[peer], scale_ref.at[me], fact_send.at[0], fact_recv.at[0], where
        ).start()
        remote(
            code_a.at[peer], part_a.at[me], part_send.at[0], part_recv.at[0], where
        ).start()

    def give_rest(i, j):
        where = target(i, j)
        remote(
            code_b.at[where[0] * 16 + where[1]], part_b.at[me],
            part_send.at[1], part_recv.at[1], where,
        ).start()

    def index(i, j):
        where = target(i, j)
        return where[0] * 16 + where[1]

    for j in range(WIDE):
        right_product(index(0, j), j)

    def work(i, c):
        for j in range(WIDE):
            right_product(index(i, j), j)

        for j in range(WIDE):
            @pl.when((i > 1) | (j > 0))
            def _():
                give(i - 1, j)
        return c

    lax.fori_loop(1, ROUNDS, work, 0)
    for j in range(WIDE):
        give(ROUNDS - 1, j)
    each(give_rest)
    part_a[me] = code_a[me]
    part_b[me] = code_b[me]
    scale_ref[me] = factor_ref[me]

    def locate(d, row):
        return jnp.where(row_lane == d, owner_ref[asked(d, 0)], row)

    place = lax.fori_loop(0, n, locate, jnp.zeros((1, LANES), jnp.int32), unroll=8)
    hot = jnp.where(
        lax.broadcasted_iota(jnp.int32, (n, LANES), 0) == place, 1.0, 0.0
    ).astype(jnp.bfloat16)
    hot = jnp.concatenate([hot, hot], axis=1)

    tiles = width // LANES

    def spread(part, first, rows, d):
        values = part[d].astype(jnp.int32).astype(jnp.float32)
        values = values * as_column(scale_ref[d], rows, first)
        hi = values.astype(jnp.bfloat16).astype(jnp.float32)
        both = jnp.concatenate([hi, values - hi], axis=0).astype(jnp.bfloat16)
        units = jnp.concatenate(
            [table_ref[asked(d, 1 + q)] for q in range(bps)], axis=0
        )
        moved = jnp.dot(both, units, preferred_element_type=jnp.float32)
        moved = moved[:rows] + moved[rows:]
        for k in range(tiles):
            spread_ref[k, pl.ds(d * PITCH + first, rows), :] = moved[:, LANES * k : LANES * (k + 1)]

    def combine(c, carry):
        at = pl.ds(c, n, stride=PITCH)
        every = jnp.concatenate([spread_ref[k, at, :] for k in range(tiles)], axis=1)
        total = jnp.dot(
            hot, jnp.concatenate(split(every), axis=0), preferred_element_type=jnp.float32
        )
        for k in range(tiles):
            total_ref[k, at, :] = total[:, LANES * k : LANES * (k + 1)]
        return carry

    for h, ((first, rows), code_ref, part, rows_ref, land_ref) in enumerate(
        zip(CHUNKS, (code_a, code_b), (part_a, part_b), (rows_a, rows_b), (land_a, land_b))
    ):
        bulk(code_ref, part, part_send.at[h], part_recv.at[h], n - 1).wait()
        if h == 0:
            bulk(factor_ref, scale_ref, fact_send.at[0], fact_recv.at[0], n - 1).wait()

        def spread_some(i, c):
            for j in range(WIDE):
                spread(part, first, rows, i * WIDE + j)
            return c

        lax.fori_loop(0, ROUNDS, spread_some, 0)
        lax.fori_loop(first, first + rows, combine, 0)

        def encode(o):
            row = jnp.concatenate(
                [total_ref[k, pl.ds(o * PITCH + first, rows), :] for k in range(tiles)], axis=1
            )
            code, factor = coded(row)
            rows_ref[o] = code.astype(jnp.int16)
            rows_scale[h, o] = as_row(factor, first)

        def deliver(i, j):
            where = target(i, j)
            peer = where[0] * 16 + where[1]
            remote(
                rows_scale.at[h, peer], land_scale.at[h, me],
                rsc_send.at[h], rsc_recv.at[h, i], where,
            ).start()
            remote(
                rows_ref.at[peer], land_ref.at[me],
                rows_send.at[h], rows_recv.at[h, i], where,
            ).start()

        for j in range(WIDE):
            encode(index(0, j))

        def emit(i, c):
            for j in range(WIDE):
                encode(index(i, j))
            for j in range(WIDE):
                @pl.when((i > 1) | (j > 0))
                def _():
                    deliver(i - 1, j)
            return c

        lax.fori_loop(1, ROUNDS, emit, 0)
        for j in range(WIDE):
            deliver(ROUNDS - 1, j)

    for h, ((first, rows), rows_ref, land_ref) in enumerate(
        zip(CHUNKS, (rows_a, rows_b), (land_a, land_b))
    ):
        def decode(code, scale, p):
            out_ref[p, first : first + rows, :] = code.astype(jnp.int32).astype(
                jnp.float32
            ) * as_column(scale, rows, first)

        def arrived(i, count):
            bulk(rows_ref, land_ref, rows_send.at[h], rows_recv.at[h, i], count).wait_recv()
            bulk(
                rows_scale.at[h], land_scale.at[h], rsc_send.at[h], rsc_recv.at[h, i], count
            ).wait_recv()

        decode(rows_ref[me], rows_scale[h, me], me)
        arrived(0, WIDE - 1)
        for j in range(1, WIDE):
            p = source(0, j)
            decode(land_ref[p], land_scale[h, p], p)

        def drain(i, c):
            arrived(i, WIDE)
            for j in range(WIDE):
                p = source(i, j)
                decode(land_ref[p], land_scale[h, p], p)
            return c

        lax.fori_loop(1, ROUNDS, drain, 0)
        bulk(rows_ref, land_ref, rows_send.at[h], rows_recv.at[h, 0], n - 1).wait_send()
        bulk(
            rows_scale.at[h], land_scale.at[h], rsc_send.at[h], rsc_recv.at[h, 0], n - 1
        ).wait_send()
    bulk(stage_ref, fetched_ref, fetch_send.at[0], fetch_recv.at[0], n - 1).wait_send()


def whole(col_slot, col_pos, request, owners, prolong, stiffness):
    slots, bps, dof, _ = stiffness.shape
    cv = prolong.shape[1]
    n = slots
    width = MAXNB * cv
    sem = pltpu.SemaphoreType.DMA
    bf16, f32, i16, i32 = jnp.bfloat16, jnp.float32, jnp.int16, jnp.int32
    return pl.pallas_call(
        whole_kernel,
        out_shape=jax.ShapeDtypeStruct((n, cv, width), f32),
        in_specs=[HBM] * 6,
        out_specs=VMEM,
        scratch_shapes=[
            pltpu.SMEM(col_slot.shape, i32),
            pltpu.SMEM(col_pos.shape, i32),
            pltpu.SMEM(request.shape, i32),
            pltpu.SMEM(owners.shape, i32),
            pltpu.VMEM(prolong.shape, bf16),
            pltpu.VMEM((8, 16, 1, LANES), i32),
            pltpu.VMEM((8, 16, 1, LANES), i32),
            pltpu.SMEM((8, 16, 1, LANES), i32),
            pltpu.VMEM((n, cv, dof), bf16),
            pltpu.VMEM((n, cv, dof), bf16),
            pltpu.VMEM(stiffness.shape, bf16),
            pltpu.VMEM((n, bps * cv, 2 * dof), bf16),
            pltpu.VMEM((WIDE, LANES, 2 * dof), bf16),
            *[pltpu.VMEM((n, rows, LANES), i16) for _, rows in CHUNKS],
            pltpu.VMEM((n, 1, LANES), f32),
            *[pltpu.VMEM((n, rows, LANES), i16) for _, rows in CHUNKS],
            pltpu.VMEM((n, 1, LANES), f32),
            pltpu.VMEM((MAXNB, SPAN, width), bf16),
            pltpu.VMEM((width // LANES, n * PITCH, LANES), f32),
            pltpu.VMEM((width // LANES, n * PITCH, LANES), f32),
            *[pltpu.VMEM((n, rows, width), i16) for _, rows in CHUNKS],
            pltpu.VMEM((len(CHUNKS), n, 1, LANES), f32),
            *[pltpu.VMEM((n, rows, width), i16) for _, rows in CHUNKS],
            pltpu.VMEM((len(CHUNKS), n, 1, LANES), f32),
            sem((1,)), sem((1,)),
            sem((1,)), sem((1,)),
            sem((1,)), sem((ROUNDS,)),
            sem((2,)), sem((2,)),
            sem((1,)), sem((1,)),
            sem((2,)), sem((2, ROUNDS)),
            sem((2,)), sem((2, ROUNDS)),
            sem((n // 16,)), sem((1,)), sem((5,)),
        ],
        compiler_params=pltpu.CompilerParams(
            collective_id=1, has_side_effects=True, vmem_limit_bytes=46 << 20
        ),
        name="whole",
    )(
        *[
            pltpu.with_memory_space_constraint(a, pltpu.HBM)
            for a in (col_slot, col_pos, request, owners, prolong, stiffness)
        ]
    )


def per_device(prolong, stiffness, request, col_slot, col_pos, coarse_owner):
    return whole(col_slot.T, col_pos.T, request, coarse_owner[:, 0], prolong, stiffness)


def solution(mesh):
    placed = (
        P(AXES, None, None),
        P(AXES, None, None, None),
        P(AXES),
        P(AXES, None),
        P(AXES, None),
        P(AXES, None),
    )
    return jax.shard_map(
        per_device, mesh=mesh, in_specs=placed, out_specs=P(AXES, None, None), check_vma=False
    )
```

```python
import functools

import jax
import jax.numpy as jnp
from jax import lax
from jax.experimental import pallas as pl
from jax.experimental.pallas import tpu as pltpu
from jax.sharding import PartitionSpec as P

MAXNB = 16
AXES = ("gx", "gy")
LANES = 128
SPAN = 32
PITCH = 28
CHUNKS = ((0, 8), (8, 16))
ROUNDS = 8
WIDE = 16
COLS = 8
ROLLED = 4
TOP = 32767.0
MESH = pl.DeviceIdType.MESH
HBM = pl.BlockSpec(memory_space=pltpu.HBM)
VMEM = pl.BlockSpec(memory_space=pltpu.VMEM)
NT = (((1,), (1,)), ((), ()))


def diagonal(rows, first):
    shape = (rows, LANES)
    return (
        lax.broadcasted_iota(jnp.int32, shape, 0) + first
        == lax.broadcasted_iota(jnp.int32, shape, 1)
    )


def as_row(column, first=0):
    return jnp.sum(
        jnp.where(diagonal(column.shape[0], first), column, 0.0), axis=0, keepdims=True
    )


def as_column(row, rows, first=0):
    return jnp.sum(jnp.where(diagonal(rows, first), row, 0.0), axis=1, keepdims=True)


def coded(values):
    top = jnp.maximum(jnp.max(jnp.abs(values), axis=1, keepdims=True), 1e-30)
    code = jnp.round(values * (TOP / top)).astype(jnp.int32)
    return code, top * (1.0 / TOP)


def split(values):
    hi = values.astype(jnp.bfloat16)
    return hi, (values - hi.astype(jnp.float32)).astype(jnp.bfloat16)


def whole_kernel(
    slot_in, pos_in, ask_in, owner_in, prolong_in, stiff_ref,
    out_ref,
    slot_ref, pos_ref, ask_ref, owner_ref, prolong_ref,
    meta_ref, mid_ref, req_ref, stage_ref, fetched_ref, mats_ref, pk_ref, cols_ref,
    code_a, code_b, factor_ref, part_a, part_b, scale_ref, table_ref, spread_ref, total_ref,
    rows_a, rows_b, rows_scale, land_a, land_b, land_scale,
    near_send, near_recv, far_send, far_recv, fetch_send, fetch_recv, part_send, part_recv, fact_send, fact_recv,
    rows_send, rows_recv, rsc_send, rsc_recv, mats_sem, req_sem, arg_sem,
):
    n, cv, dof = fetched_ref.shape
    bps = mats_ref.shape[1]
    width = out_ref.shape[2]
    gx, gy = lax.axis_index("gx"), lax.axis_index("gy")
    me = gx * 16 + gy
    z, core = gx // 2, lax.rem(gx, 2)
    x, y = gy // 4, lax.rem(gy, 4)
    to_gy = [lax.rem(x + s // 4, 4) * 4 + lax.rem(y + s % 4, 4) for s in range(WIDE)]
    from_gy = [lax.rem(x + 4 - s // 4, 4) * 4 + lax.rem(y + 4 - s % 4, 4) for s in range(WIDE)]

    def shift(r):
        t = r // 2
        dz = 2 + t - 3 * (t // 2) - 2 * (t // 3)
        other = lax.rem(core + 1 + r, 2)
        return lax.rem(z + dz, 4) * 2 + other, lax.rem(z + 4 - dz, 4) * 2 + other

    def targets(r):
        row, _ = shift(r)
        return [(row, to_gy[s]) for s in range(WIDE)]

    def sources(r):
        _, row = shift(r)
        return [row * 16 + from_gy[s] for s in range(WIDE)]

    def each(fn):
        def body(r, c):
            for where in targets(r):
                fn(r, where)
            return c

        lax.fori_loop(0, ROUNDS - 1, body, 0)
        for where in targets(ROUNDS - 1)[1:]:
            fn(ROUNDS - 1, where)

    def remote(src, dst, send_sem, recv_sem, where):
        return pltpu.make_async_remote_copy(
            src_ref=src, dst_ref=dst, send_sem=send_sem, recv_sem=recv_sem,
            device_id=where, device_id_type=MESH,
        )

    def bulk(src, dst, send_sem, recv_sem, count):
        return remote(
            src.at[pl.ds(0, count)], dst.at[pl.ds(0, count)], send_sem, recv_sem, (gx, gy)
        )

    small = [
        pltpu.make_async_copy(src, dst, arg_sem.at[k])
        for k, (src, dst) in enumerate(
            (
                (ask_in, ask_ref), (pos_in, pos_ref), (slot_in, slot_ref),
                (owner_in, owner_ref), (prolong_in, prolong_ref),
            )
        )
    ]
    for copy in small:
        copy.start()
    loads = [
        pltpu.make_async_copy(
            stiff_ref.at[pl.ds(b * 16, 16)], mats_ref.at[pl.ds(b * 16, 16)], mats_sem.at[b]
        )
        for b in range(n // 16)
    ]
    for copy in loads:
        copy.start()

    barrier = pltpu.get_barrier_semaphore()
    near = [(shift(r)[0], gy) for r in range(ROUNDS - 1)]
    far = [(gx, g) for g in to_gy[1:]]
    for where in near + far:
        pl.semaphore_signal(barrier, inc=1, device_id=where, device_id_type=MESH)

    row_lane = lax.broadcasted_iota(jnp.int32, (1, LANES), 1)

    def describe(h, c):
        for g in range(8):
            p = g * 16 + h
            row = jnp.where(row_lane == 0, ask_ref[p], 0)
            for q in range(bps):
                row = jnp.where(row_lane == 1 + q, pos_ref[q, p], row)
            meta_ref[g, h] = row
        return c

    for copy in small[:2]:
        copy.wait()
    lax.fori_loop(0, 16, describe, 0)
    mid_ref[gx] = meta_ref[gx]
    cols_ref[...] = jnp.zeros_like(cols_ref)
    unit_row = lax.broadcasted_iota(jnp.int32, (SPAN, width), 0)
    unit_col = lax.broadcasted_iota(jnp.int32, (SPAN, width), 1)
    for k in range(MAXNB):
        unit = (unit_row < cv) & (unit_col == unit_row + cv * k)
        table_ref[k] = jnp.where(unit, 1.0, 0.0).astype(jnp.bfloat16)
    pl.semaphore_wait(barrier, 22)
    for where in near:
        remote(
            meta_ref.at[where[0]], mid_ref.at[gx], near_send.at[0], near_recv.at[0], where
        ).start()
    bulk(meta_ref, mid_ref, near_send.at[0], near_recv.at[0], 7).wait()
    for where in far:
        remote(
            mid_ref.at[:, where[1]], req_ref.at[:, gy], far_send.at[0], far_recv.at[0], where
        ).start()
    to_scalars = pltpu.make_async_copy(mid_ref.at[:, gy], req_ref.at[:, gy], req_sem.at[0])
    to_scalars.start()
    remote(
        mid_ref.at[:, pl.ds(0, 15)], req_ref.at[:, pl.ds(0, 15)],
        far_send.at[0], far_recv.at[0], (gx, gy),
    ).wait()
    for copy in small[2:]:
        copy.wait()
    to_scalars.wait()

    def fill(g, c):
        for h in range(16):
            stage_ref[g * 16 + h] = prolong_ref[req_ref[g, h, 0, 0]]
        return c

    lax.fori_loop(0, 8, fill, 0)

    def answer(r, where):
        remote(
            stage_ref.at[where[0] * 16 + where[1]], fetched_ref.at[me],
            fetch_send.at[0], fetch_recv.at[r], where,
        ).start()

    each(answer)
    fetched_ref[me] = prolong_ref[req_ref[gx, gy, 0, 0]]
    for copy in loads:
        copy.wait()

    def left_product(t):
        rows = fetched_ref[t]
        parts = []
        for h in range(bps // 2):
            pair = jnp.concatenate([mats_ref[t, 2 * h], mats_ref[t, 2 * h + 1]], axis=1)
            prod = jnp.dot(rows, pair, preferred_element_type=jnp.float32)
            parts += [prod[:, 0:dof], prod[:, dof : 2 * dof]]
        hi, lo = split(jnp.concatenate(parts, axis=0))
        pk_ref[t, :, 0:dof] = hi
        pk_ref[t, :, dof : 2 * dof] = lo

    def take(r, c):
        bulk(stage_ref, fetched_ref, fetch_send.at[0], fetch_recv.at[r], WIDE).wait_recv()
        for t in sources(r):
            left_product(t)
        return c

    lax.fori_loop(0, ROUNDS - 1, take, 0)
    bulk(
        stage_ref, fetched_ref, fetch_send.at[0], fetch_recv.at[ROUNDS - 1], WIDE - 1
    ).wait_recv()
    for t in sources(ROUNDS - 1):
        left_product(t)

    lane = lax.broadcasted_iota(jnp.int32, (cv, LANES), 1)

    def right_product(t, u):
        for q in range(bps):
            block = fetched_ref[slot_ref[q, t]]
            cols_ref[u, SPAN * q : SPAN * q + cv, 0:dof] = block
            cols_ref[u, SPAN * q : SPAN * q + cv, dof : 2 * dof] = block
        prod = lax.dot_general(pk_ref[t], cols_ref[u], NT, preferred_element_type=jnp.float32)
        one = prod[(bps - 1) * cv :]
        for q in range(bps - 2, -1, -1):
            one = jnp.where(lane < SPAN * (q + 1), prod[q * cv : (q + 1) * cv], one)
        code, factor = coded(one)
        for (first, rows), ref in zip(CHUNKS, (code_a, code_b)):
            ref[t] = code[first : first + rows].astype(jnp.int16)
        factor_ref[t] = as_row(factor)

    def give(where):
        peer = where[0] * 16 + where[1]
        remote(
            factor_ref.at[peer], scale_ref.at[me], fact_send.at[0], fact_recv.at[0], where
        ).start()
        remote(
            code_a.at[peer], part_a.at[me], part_send.at[0], part_recv.at[0], where
        ).start()

    def give_rest(r, where):
        remote(
            code_b.at[where[0] * 16 + where[1]], part_b.at[me],
            part_send.at[1], part_recv.at[1], where,
        ).start()

    def multiply(r):
        for s, where in enumerate(targets(r)):
            right_product(where[0] * 16 + where[1], s % COLS)

    def work(r, c):
        multiply(r)
        for where in targets(r - 1):
            give(where)
        return c

    multiply(0)
    lax.fori_loop(1, ROUNDS, work, 0)
    for where in targets(ROUNDS - 1)[1:]:
        give(where)
    each(give_rest)
    part_a[me] = code_a[me]
    part_b[me] = code_b[me]
    scale_ref[me] = factor_ref[me]

    def locate(g, row):
        for h in range(16):
            row = jnp.where(row_lane == g * 16 + h, owner_ref[req_ref[g, h, 0, 0]], row)
        return row

    place = lax.fori_loop(0, 8, locate, jnp.zeros((1, LANES), jnp.int32))
    hot = jnp.where(
        lax.broadcasted_iota(jnp.int32, (n, LANES), 0) == place, 1.0, 0.0
    ).astype(jnp.bfloat16)
    hot = jnp.concatenate([hot, hot], axis=1)

    tiles = width // LANES

    lane_row = lax.broadcasted_iota(jnp.int32, (1, LANES), 1)
    blocks = [(lane_row + LANES * k) // cv for k in range(tiles)]

    def spread(part, first, rows, g, h):
        d = g * 16 + h
        values = part[d].astype(jnp.int32).astype(jnp.float32)
        values = values * as_column(scale_ref[d], rows, first)
        pos = [req_ref[g, h, 0, 1 + q] for q in range(bps)]
        if h % ROLLED:
            hi = values.astype(jnp.bfloat16).astype(jnp.float32)
            both = jnp.concatenate([hi, values - hi], axis=0).astype(jnp.bfloat16)
            units = jnp.concatenate([table_ref[p] for p in pos], axis=0)
            moved = jnp.dot(both, units, preferred_element_type=jnp.float32)
            moved = moved[:rows] + moved[rows:]
            moved = [moved[:, LANES * k : LANES * (k + 1)] for k in range(tiles)]
        else:
            moved = [jnp.zeros((rows, LANES), jnp.float32)] * tiles
            for q, p in enumerate(pos):
                turned = pltpu.roll(values, lax.rem(p * cv - SPAN * q + LANES, LANES), 1)
                moved = [jnp.where(k == p, turned, m) for k, m in zip(blocks, moved)]
        for k in range(tiles):
            spread_ref[k, pl.ds(d * PITCH + first, rows), :] = moved[k]

    def combine(c, carry):
        at = pl.ds(c, n, stride=PITCH)
        every = jnp.concatenate([spread_ref[k, at, :] for k in range(tiles)], axis=1)
        total = jnp.dot(
            hot, jnp.concatenate(split(every), axis=0), preferred_element_type=jnp.float32
        )
        for k in range(tiles):
            total_ref[k, at, :] = total[:, LANES * k : LANES * (k + 1)]
        return carry

    for h, ((first, rows), code_ref, part, rows_ref, land_ref) in enumerate(
        zip(CHUNKS, (code_a, code_b), (part_a, part_b), (rows_a, rows_b), (land_a, land_b))
    ):
        bulk(code_ref, part, part_send.at[h], part_recv.at[h], n - 1).wait()
        if h == 0:
            bulk(factor_ref, scale_ref, fact_send.at[0], fact_recv.at[0], n - 1).wait()

        def spread_some(g, c):
            for j in range(16):
                spread(part, first, rows, g, j)
            return c

        lax.fori_loop(0, 8, spread_some, 0)
        lax.fori_loop(first, first + rows, combine, 0)

        def encode(o):
            row = jnp.concatenate(
                [total_ref[k, pl.ds(o * PITCH + first, rows), :] for k in range(tiles)], axis=1
            )
            code, factor = coded(row)
            rows_ref[o] = code.astype(jnp.int16)
            rows_scale[h, o] = as_row(factor, first)

        def deliver(r, where):
            peer = where[0] * 16 + where[1]
            remote(
                rows_scale.at[h, peer], land_scale.at[h, me],
                rsc_send.at[h], rsc_recv.at[h, r], where,
            ).start()
            remote(
                rows_ref.at[peer], land_ref.at[me],
                rows_send.at[h], rows_recv.at[h, r], where,
            ).start()

        def encode_all(r):
            for where in targets(r):
                encode(where[0] * 16 + where[1])

        def emit(r, c):
            encode_all(r)
            for where in targets(r - 1):
                deliver(r - 1, where)
            return c

        encode_all(0)
        lax.fori_loop(1, ROUNDS, emit, 0)
        for where in targets(ROUNDS - 1)[1:]:
            deliver(ROUNDS - 1, where)

    for h, ((first, rows), rows_ref, land_ref) in enumerate(
        zip(CHUNKS, (rows_a, rows_b), (land_a, land_b))
    ):
        def decode(code, scale, p):
            out_ref[p, first : first + rows, :] = code.astype(jnp.int32).astype(
                jnp.float32
            ) * as_column(scale, rows, first)

        def arrived(i, count):
            bulk(rows_ref, land_ref, rows_send.at[h], rows_recv.at[h, i], count).wait_recv()
            bulk(
                rows_scale.at[h], land_scale.at[h], rsc_send.at[h], rsc_recv.at[h, i], count
            ).wait_recv()

        decode(rows_ref[me], rows_scale[h, me], me)

        def drain(r, c):
            arrived(r, WIDE)
            for p in sources(r):
                decode(land_ref[p], land_scale[h, p], p)
            return c

        lax.fori_loop(0, ROUNDS - 1, drain, 0)
        arrived(ROUNDS - 1, WIDE - 1)
        for p in sources(ROUNDS - 1)[1:]:
            decode(land_ref[p], land_scale[h, p], p)
        bulk(rows_ref, land_ref, rows_send.at[h], rows_recv.at[h, 0], n - 1).wait_send()
        bulk(
            rows_scale.at[h], land_scale.at[h], rsc_send.at[h], rsc_recv.at[h, 0], n - 1
        ).wait_send()
    bulk(stage_ref, fetched_ref, fetch_send.at[0], fetch_recv.at[0], n - 1).wait_send()


def whole(col_slot, col_pos, request, owners, prolong, stiffness):
    slots, bps, dof, _ = stiffness.shape
    cv = prolong.shape[1]
    n = slots
    width = MAXNB * cv
    sem = pltpu.SemaphoreType.DMA
    bf16, f32, i16, i32 = jnp.bfloat16, jnp.float32, jnp.int16, jnp.int32
    return pl.pallas_call(
        whole_kernel,
        out_shape=jax.ShapeDtypeStruct((n, cv, width), f32),
        in_specs=[HBM] * 6,
        out_specs=VMEM,
        scratch_shapes=[
            pltpu.SMEM(col_slot.shape, i32),
            pltpu.SMEM(col_pos.shape, i32),
            pltpu.SMEM(request.shape, i32),
            pltpu.SMEM(owners.shape, i32),
            pltpu.VMEM(prolong.shape, bf16),
            pltpu.VMEM((8, 16, 1, LANES), i32),
            pltpu.VMEM((8, 16, 1, LANES), i32),
            pltpu.SMEM((8, 16, 1, LANES), i32),
            pltpu.VMEM((n, cv, dof), bf16),
            pltpu.VMEM((n, cv, dof), bf16),
            pltpu.VMEM(stiffness.shape, bf16),
            pltpu.VMEM((n, bps * cv, 2 * dof), bf16),
            pltpu.VMEM((COLS, LANES, 2 * dof), bf16),
            *[pltpu.VMEM((n, rows, LANES), i16) for _, rows in CHUNKS],
            pltpu.VMEM((n, 1, LANES), f32),
            *[pltpu.VMEM((n, rows, LANES), i16) for _, rows in CHUNKS],
            pltpu.VMEM((n, 1, LANES), f32),
            pltpu.VMEM((MAXNB, SPAN, width), bf16),
            pltpu.VMEM((width // LANES, n * PITCH, LANES), f32),
            pltpu.VMEM((width // LANES, n * PITCH, LANES), f32),
            *[pltpu.VMEM((n, rows, width), i16) for _, rows in CHUNKS],
            pltpu.VMEM((len(CHUNKS), n, 1, LANES), f32),
            *[pltpu.VMEM((n, rows, width), i16) for _, rows in CHUNKS],
            pltpu.VMEM((len(CHUNKS), n, 1, LANES), f32),
            sem((1,)), sem((1,)),
            sem((1,)), sem((1,)),
            sem((1,)), sem((ROUNDS,)),
            sem((2,)), sem((2,)),
            sem((1,)), sem((1,)),
            sem((2,)), sem((2, ROUNDS)),
            sem((2,)), sem((2, ROUNDS)),
            sem((n // 16,)), sem((1,)), sem((5,)),
        ],
        compiler_params=pltpu.CompilerParams(
            collective_id=1, has_side_effects=True, vmem_limit_bytes=46 << 20
        ),
        name="whole",
    )(
        *[
            pltpu.with_memory_space_constraint(a, pltpu.HBM)
            for a in (col_slot, col_pos, request, owners, prolong, stiffness)
        ]
    )


def per_device(prolong, stiffness, request, col_slot, col_pos, coarse_owner):
    return whole(col_slot.T, col_pos.T, request, coarse_owner[:, 0], prolong, stiffness)


def solution(mesh):
    placed = (
        P(AXES, None, None),
        P(AXES, None, None, None),
        P(AXES),
        P(AXES, None),
        P(AXES, None),
        P(AXES, None),
    )
    return jax.shard_map(
        per_device, mesh=mesh, in_specs=placed, out_specs=P(AXES, None, None), check_vma=False
    )
```

```python
import functools

import jax
import jax.numpy as jnp
from jax import lax
from jax.experimental import pallas as pl
from jax.experimental.pallas import tpu as pltpu
from jax.sharding import PartitionSpec as P

MAXNB = 16
AXES = ("gx", "gy")
LANES = 128
SPAN = 32
PITCH = 28
CHUNKS = ((0, 8), (8, 16))
ROUNDS = 8
WIDE = 16
COLS = 8
ROLLED = 4
TOP = 32767.0
MESH = pl.DeviceIdType.MESH
HBM = pl.BlockSpec(memory_space=pltpu.HBM)
VMEM = pl.BlockSpec(memory_space=pltpu.VMEM)
NT = (((1,), (1,)), ((), ()))


def diagonal(rows, first):
    shape = (rows, LANES)
    return (
        lax.broadcasted_iota(jnp.int32, shape, 0) + first
        == lax.broadcasted_iota(jnp.int32, shape, 1)
    )


def as_row(column, first=0):
    return jnp.sum(
        jnp.where(diagonal(column.shape[0], first), column, 0.0), axis=0, keepdims=True
    )


def as_column(row, rows, first=0):
    return jnp.sum(jnp.where(diagonal(rows, first), row, 0.0), axis=1, keepdims=True)


def coded(values):
    top = jnp.maximum(jnp.max(jnp.abs(values), axis=1, keepdims=True), 1e-30)
    code = jnp.round(values * (TOP / top)).astype(jnp.int32)
    return code, top * (1.0 / TOP)


def split(values):
    hi = values.astype(jnp.bfloat16)
    return hi, (values - hi.astype(jnp.float32)).astype(jnp.bfloat16)


def whole_kernel(
    slot_in, pos_in, ask_in, owner_in, prolong_in, stiff_ref,
    out_ref,
    slot_ref, pos_ref, ask_ref, owner_ref, prolong_ref,
    meta_ref, mid_ref, req_ref, stage_ref, fetched_ref, mats_ref, pk_ref, cols_ref,
    code_a, code_b, factor_ref, part_a, part_b, scale_ref, table_ref, spread_ref, total_ref,
    rows_a, rows_b, rows_scale, land_a, land_b, land_scale,
    near_send, near_recv, far_send, far_recv, fetch_send, fetch_recv, part_send, part_recv, fact_send, fact_recv,
    rows_send, rows_recv, rsc_send, rsc_recv, mats_sem, req_sem, arg_sem,
):
    n, cv, dof = fetched_ref.shape
    bps = mats_ref.shape[1]
    width = out_ref.shape[2]
    gx, gy = lax.axis_index("gx"), lax.axis_index("gy")
    me = gx * 16 + gy
    z, core = gx // 2, lax.rem(gx, 2)
    x, y = gy // 4, lax.rem(gy, 4)
    to_gy = [lax.rem(x + s // 4, 4) * 4 + lax.rem(y + s % 4, 4) for s in range(WIDE)]
    from_gy = [lax.rem(x + 4 - s // 4, 4) * 4 + lax.rem(y + 4 - s % 4, 4) for s in range(WIDE)]

    def shift(r):
        u = r % 4
        dz = 2 - u + 3 * (u // 2) - 2 * (u // 3)
        other = lax.rem(core + 1 + u % 2 - u // 3 + r // 4, 2)
        return lax.rem(z + dz, 4) * 2 + other, lax.rem(z + 4 - dz, 4) * 2 + other

    def targets(r):
        row, _ = shift(r)
        return [(row, to_gy[s]) for s in range(WIDE)]

    def sources(r):
        _, row = shift(r)
        return [row * 16 + from_gy[s] for s in range(WIDE)]

    def each(fn):
        def body(r, c):
            for where in targets(r):
                fn(r, where)
            return c

        lax.fori_loop(0, ROUNDS - 1, body, 0)
        for where in targets(ROUNDS - 1)[1:]:
            fn(ROUNDS - 1, where)

    def remote(src, dst, send_sem, recv_sem, where):
        return pltpu.make_async_remote_copy(
            src_ref=src, dst_ref=dst, send_sem=send_sem, recv_sem=recv_sem,
            device_id=where, device_id_type=MESH,
        )

    def bulk(src, dst, send_sem, recv_sem, count):
        return remote(
            src.at[pl.ds(0, count)], dst.at[pl.ds(0, count)], send_sem, recv_sem, (gx, gy)
        )

    small = [
        pltpu.make_async_copy(src, dst, arg_sem.at[k])
        for k, (src, dst) in enumerate(
            (
                (ask_in, ask_ref), (pos_in, pos_ref), (slot_in, slot_ref),
                (owner_in, owner_ref), (prolong_in, prolong_ref),
            )
        )
    ]
    for copy in small:
        copy.start()
    loads = [
        pltpu.make_async_copy(
            stiff_ref.at[pl.ds(b * 16, 16)], mats_ref.at[pl.ds(b * 16, 16)], mats_sem.at[b]
        )
        for b in range(n // 16)
    ]
    for copy in loads:
        copy.start()

    barrier = pltpu.get_barrier_semaphore()
    near = [(shift(r)[0], gy) for r in range(ROUNDS - 1)]
    far = [(gx, g) for g in to_gy[1:]]
    for where in near + far:
        pl.semaphore_signal(barrier, inc=1, device_id=where, device_id_type=MESH)

    row_lane = lax.broadcasted_iota(jnp.int32, (1, LANES), 1)

    def describe(h, c):
        for g in range(8):
            p = g * 16 + h
            row = jnp.where(row_lane == 0, ask_ref[p], 0)
            for q in range(bps):
                row = jnp.where(row_lane == 1 + q, pos_ref[q, p], row)
            meta_ref[g, h] = row
        return c

    for copy in small[:2]:
        copy.wait()
    lax.fori_loop(0, 16, describe, 0)
    mid_ref[gx] = meta_ref[gx]
    cols_ref[...] = jnp.zeros_like(cols_ref)
    unit_row = lax.broadcasted_iota(jnp.int32, (SPAN, width), 0)
    unit_col = lax.broadcasted_iota(jnp.int32, (SPAN, width), 1)
    for k in range(MAXNB):
        unit = (unit_row < cv) & (unit_col == unit_row + cv * k)
        table_ref[k] = jnp.where(unit, 1.0, 0.0).astype(jnp.bfloat16)
    pl.semaphore_wait(barrier, 22)
    for where in near:
        remote(
            meta_ref.at[where[0]], mid_ref.at[gx], near_send.at[0], near_recv.at[0], where
        ).start()
    bulk(meta_ref, mid_ref, near_send.at[0], near_recv.at[0], 7).wait()
    for where in far:
        remote(
            mid_ref.at[:, where[1]], req_ref.at[:, gy], far_send.at[0], far_recv.at[0], where
        ).start()
    to_scalars = pltpu.make_async_copy(mid_ref.at[:, gy], req_ref.at[:, gy], req_sem.at[0])
    to_scalars.start()
    remote(
        mid_ref.at[:, pl.ds(0, 15)], req_ref.at[:, pl.ds(0, 15)],
        far_send.at[0], far_recv.at[0], (gx, gy),
    ).wait()
    for copy in small[2:]:
        copy.wait()
    to_scalars.wait()

    def fill(g, c):
        for h in range(16):
            stage_ref[g * 16 + h] = prolong_ref[req_ref[g, h, 0, 0]]
        return c

    lax.fori_loop(0, 8, fill, 0)

    def answer(r, where):
        remote(
            stage_ref.at[where[0] * 16 + where[1]], fetched_ref.at[me],
            fetch_send.at[0], fetch_recv.at[r], where,
        ).start()

    each(answer)
    fetched_ref[me] = prolong_ref[req_ref[gx, gy, 0, 0]]
    for copy in loads:
        copy.wait()

    def left_product(t):
        rows = fetched_ref[t]
        parts = []
        for h in range(bps // 2):
            pair = jnp.concatenate([mats_ref[t, 2 * h], mats_ref[t, 2 * h + 1]], axis=1)
            prod = jnp.dot(rows, pair, preferred_element_type=jnp.float32)
            parts += [prod[:, 0:dof], prod[:, dof : 2 * dof]]
        hi, lo = split(jnp.concatenate(parts, axis=0))
        pk_ref[t, :, 0:dof] = hi
        pk_ref[t, :, dof : 2 * dof] = lo

    def take(r, c):
        bulk(stage_ref, fetched_ref, fetch_send.at[0], fetch_recv.at[r], WIDE).wait_recv()
        for t in sources(r):
            left_product(t)
        return c

    lax.fori_loop(0, ROUNDS - 1, take, 0)
    bulk(
        stage_ref, fetched_ref, fetch_send.at[0], fetch_recv.at[ROUNDS - 1], WIDE - 1
    ).wait_recv()
    for t in sources(ROUNDS - 1):
        left_product(t)

    lane = lax.broadcasted_iota(jnp.int32, (cv, LANES), 1)

    def right_product(t, u):
        for q in range(bps):
            block = fetched_ref[slot_ref[q, t]]
            cols_ref[u, SPAN * q : SPAN * q + cv, 0:dof] = block
            cols_ref[u, SPAN * q : SPAN * q + cv, dof : 2 * dof] = block
        prod = lax.dot_general(pk_ref[t], cols_ref[u], NT, preferred_element_type=jnp.float32)
        one = prod[(bps - 1) * cv :]
        for q in range(bps - 2, -1, -1):
            one = jnp.where(lane < SPAN * (q + 1), prod[q * cv : (q + 1) * cv], one)
        code, factor = coded(one)
        for (first, rows), ref in zip(CHUNKS, (code_a, code_b)):
            ref[t] = code[first : first + rows].astype(jnp.int16)
        factor_ref[t] = as_row(factor)

    def give(where):
        peer = where[0] * 16 + where[1]
        remote(
            factor_ref.at[peer], scale_ref.at[me], fact_send.at[0], fact_recv.at[0], where
        ).start()
        remote(
            code_a.at[peer], part_a.at[me], part_send.at[0], part_recv.at[0], where
        ).start()

    def give_rest(r, where):
        remote(
            code_b.at[where[0] * 16 + where[1]], part_b.at[me],
            part_send.at[1], part_recv.at[1], where,
        ).start()

    def multiply(r):
        for s, where in enumerate(targets(r)):
            right_product(where[0] * 16 + where[1], s % COLS)

    def work(r, c):
        multiply(r)
        for where in targets(r - 1):
            give(where)
        return c

    multiply(0)
    lax.fori_loop(1, ROUNDS, work, 0)
    for where in targets(ROUNDS - 1)[1:]:
        give(where)
    each(give_rest)
    part_a[me] = code_a[me]
    part_b[me] = code_b[me]
    scale_ref[me] = factor_ref[me]

    def locate(g, row):
        for h in range(16):
            row = jnp.where(row_lane == g * 16 + h, owner_ref[req_ref[g, h, 0, 0]], row)
        return row

    place = lax.fori_loop(0, 8, locate, jnp.zeros((1, LANES), jnp.int32))
    hot = jnp.where(
        lax.broadcasted_iota(jnp.int32, (n, LANES), 0) == place, 1.0, 0.0
    ).astype(jnp.bfloat16)
    hot = jnp.concatenate([hot, hot], axis=1)

    tiles = width // LANES

    lane_row = lax.broadcasted_iota(jnp.int32, (1, LANES), 1)
    blocks = [(lane_row + LANES * k) // cv for k in range(tiles)]

    def spread(part, first, rows, g, h):
        d = g * 16 + h
        values = part[d].astype(jnp.int32).astype(jnp.float32)
        values = values * as_column(scale_ref[d], rows, first)
        pos = [req_ref[g, h, 0, 1 + q] for q in range(bps)]
        if h % ROLLED:
            hi = values.astype(jnp.bfloat16).astype(jnp.float32)
            both = jnp.concatenate([hi, values - hi], axis=0).astype(jnp.bfloat16)
            units = jnp.concatenate([table_ref[p] for p in pos], axis=0)
            moved = jnp.dot(both, units, preferred_element_type=jnp.float32)
            moved = moved[:rows] + moved[rows:]
            moved = [moved[:, LANES * k : LANES * (k + 1)] for k in range(tiles)]
        else:
            moved = [jnp.zeros((rows, LANES), jnp.float32)] * tiles
            for q, p in enumerate(pos):
                turned = pltpu.roll(values, lax.rem(p * cv - SPAN * q + LANES, LANES), 1)
                moved = [jnp.where(k == p, turned, m) for k, m in zip(blocks, moved)]
        for k in range(tiles):
            spread_ref[k, pl.ds(d * PITCH + first, rows), :] = moved[k]

    def combine(c, carry):
        at = pl.ds(c, n, stride=PITCH)
        every = jnp.concatenate([spread_ref[k, at, :] for k in range(tiles)], axis=1)
        total = jnp.dot(
            hot, jnp.concatenate(split(every), axis=0), preferred_element_type=jnp.float32
        )
        for k in range(tiles):
            total_ref[k, at, :] = total[:, LANES * k : LANES * (k + 1)]
        return carry

    for h, ((first, rows), code_ref, part, rows_ref, land_ref) in enumerate(
        zip(CHUNKS, (code_a, code_b), (part_a, part_b), (rows_a, rows_b), (land_a, land_b))
    ):
        bulk(code_ref, part, part_send.at[h], part_recv.at[h], n - 1).wait()
        if h == 0:
            bulk(factor_ref, scale_ref, fact_send.at[0], fact_recv.at[0], n - 1).wait()

        def spread_some(g, c):
            for j in range(16):
                spread(part, first, rows, g, j)
            return c

        lax.fori_loop(0, 8, spread_some, 0)
        lax.fori_loop(first, first + rows, combine, 0)

        def encode(o):
            row = jnp.concatenate(
                [total_ref[k, pl.ds(o * PITCH + first, rows), :] for k in range(tiles)], axis=1
            )
            code, factor = coded(row)
            rows_ref[o] = code.astype(jnp.int16)
            rows_scale[h, o] = as_row(factor, first)

        def deliver(r, where):
            peer = where[0] * 16 + where[1]
            remote(
                rows_scale.at[h, peer], land_scale.at[h, me],
                rsc_send.at[h], rsc_recv.at[h, r], where,
            ).start()
            remote(
                rows_ref.at[peer], land_ref.at[me],
                rows_send.at[h], rows_recv.at[h, r], where,
            ).start()

        def encode_all(r):
            for where in targets(r):
                encode(where[0] * 16 + where[1])

        def emit(r, c):
            encode_all(r)
            for where in targets(r - 1):
                deliver(r - 1, where)
            return c

        encode_all(0)
        lax.fori_loop(1, ROUNDS, emit, 0)
        for where in targets(ROUNDS - 1)[1:]:
            deliver(ROUNDS - 1, where)

    for h, ((first, rows), rows_ref, land_ref) in enumerate(
        zip(CHUNKS, (rows_a, rows_b), (land_a, land_b))
    ):
        def decode(code, scale, p):
            out_ref[p, first : first + rows, :] = code.astype(jnp.int32).astype(
                jnp.float32
            ) * as_column(scale, rows, first)

        def arrived(i, count):
            bulk(rows_ref, land_ref, rows_send.at[h], rows_recv.at[h, i], count).wait_recv()
            bulk(
                rows_scale.at[h], land_scale.at[h], rsc_send.at[h], rsc_recv.at[h, i], count
            ).wait_recv()

        decode(rows_ref[me], rows_scale[h, me], me)

        def drain(r, c):
            arrived(r, WIDE)
            for p in sources(r):
                decode(land_ref[p], land_scale[h, p], p)
            return c

        lax.fori_loop(0, ROUNDS - 1, drain, 0)
        arrived(ROUNDS - 1, WIDE - 1)
        for p in sources(ROUNDS - 1)[1:]:
            decode(land_ref[p], land_scale[h, p], p)
        bulk(rows_ref, land_ref, rows_send.at[h], rows_recv.at[h, 0], n - 1).wait_send()
        bulk(
            rows_scale.at[h], land_scale.at[h], rsc_send.at[h], rsc_recv.at[h, 0], n - 1
        ).wait_send()
    bulk(stage_ref, fetched_ref, fetch_send.at[0], fetch_recv.at[0], n - 1).wait_send()


def whole(col_slot, col_pos, request, owners, prolong, stiffness):
    slots, bps, dof, _ = stiffness.shape
    cv = prolong.shape[1]
    n = slots
    width = MAXNB * cv
    sem = pltpu.SemaphoreType.DMA
    bf16, f32, i16, i32 = jnp.bfloat16, jnp.float32, jnp.int16, jnp.int32
    return pl.pallas_call(
        whole_kernel,
        out_shape=jax.ShapeDtypeStruct((n, cv, width), f32),
        in_specs=[HBM] * 6,
        out_specs=VMEM,
        scratch_shapes=[
            pltpu.SMEM(col_slot.shape, i32),
            pltpu.SMEM(col_pos.shape, i32),
            pltpu.SMEM(request.shape, i32),
            pltpu.SMEM(owners.shape, i32),
            pltpu.VMEM(prolong.shape, bf16),
            pltpu.VMEM((8, 16, 1, LANES), i32),
            pltpu.VMEM((8, 16, 1, LANES), i32),
            pltpu.SMEM((8, 16, 1, LANES), i32),
            pltpu.VMEM((n, cv, dof), bf16),
            pltpu.VMEM((n, cv, dof), bf16),
            pltpu.VMEM(stiffness.shape, bf16),
            pltpu.VMEM((n, bps * cv, 2 * dof), bf16),
            pltpu.VMEM((COLS, LANES, 2 * dof), bf16),
            *[pltpu.VMEM((n, rows, LANES), i16) for _, rows in CHUNKS],
            pltpu.VMEM((n, 1, LANES), f32),
            *[pltpu.VMEM((n, rows, LANES), i16) for _, rows in CHUNKS],
            pltpu.VMEM((n, 1, LANES), f32),
            pltpu.VMEM((MAXNB, SPAN, width), bf16),
            pltpu.VMEM((width // LANES, n * PITCH, LANES), f32),
            pltpu.VMEM((width // LANES, n * PITCH, LANES), f32),
            *[pltpu.VMEM((n, rows, width), i16) for _, rows in CHUNKS],
            pltpu.VMEM((len(CHUNKS), n, 1, LANES), f32),
            *[pltpu.VMEM((n, rows, width), i16) for _, rows in CHUNKS],
            pltpu.VMEM((len(CHUNKS), n, 1, LANES), f32),
            sem((1,)), sem((1,)),
            sem((1,)), sem((1,)),
            sem((1,)), sem((ROUNDS,)),
            sem((2,)), sem((2,)),
            sem((1,)), sem((1,)),
            sem((2,)), sem((2, ROUNDS)),
            sem((2,)), sem((2, ROUNDS)),
            sem((n // 16,)), sem((1,)), sem((5,)),
        ],
        compiler_params=pltpu.CompilerParams(
            collective_id=1, has_side_effects=True, vmem_limit_bytes=46 << 20
        ),
        name="whole",
    )(
        *[
            pltpu.with_memory_space_constraint(a, pltpu.HBM)
            for a in (col_slot, col_pos, request, owners, prolong, stiffness)
        ]
    )


def per_device(prolong, stiffness, request, col_slot, col_pos, coarse_owner):
    return whole(col_slot.T, col_pos.T, request, coarse_owner[:, 0], prolong, stiffness)


def solution(mesh):
    placed = (
        P(AXES, None, None),
        P(AXES, None, None, None),
        P(AXES),
        P(AXES, None),
        P(AXES, None),
        P(AXES, None),
    )
    return jax.shard_map(
        per_device, mesh=mesh, in_specs=placed, out_specs=P(AXES, None, None), check_vma=False
    )
```

```python
import functools

import jax
import jax.numpy as jnp
from jax import lax
from jax.experimental import pallas as pl
from jax.experimental.pallas import tpu as pltpu
from jax.sharding import PartitionSpec as P

MAXNB = 16
AXES = ("gx", "gy")
LANES = 128
SPAN = 32
PITCH = 28
CHUNKS = ((0, 8), (8, 16))
ROUNDS = 8
WIDE = 16
TURNS = (0, 7, 14, 5, 12, 3, 10, 1, 8, 15, 6, 13, 4, 11, 2, 9)
COLS = 8
ROLLED = 4
TOP = 32767.0
MESH = pl.DeviceIdType.MESH
HBM = pl.BlockSpec(memory_space=pltpu.HBM)
VMEM = pl.BlockSpec(memory_space=pltpu.VMEM)
NT = (((1,), (1,)), ((), ()))


def diagonal(rows, first):
    shape = (rows, LANES)
    return (
        lax.broadcasted_iota(jnp.int32, shape, 0) + first
        == lax.broadcasted_iota(jnp.int32, shape, 1)
    )


def as_row(column, first=0):
    return jnp.sum(
        jnp.where(diagonal(column.shape[0], first), column, 0.0), axis=0, keepdims=True
    )


def as_column(row, rows, first=0):
    return jnp.sum(jnp.where(diagonal(rows, first), row, 0.0), axis=1, keepdims=True)


def coded(values):
    top = jnp.maximum(jnp.max(jnp.abs(values), axis=1, keepdims=True), 1e-30)
    code = jnp.round(values * (TOP / top)).astype(jnp.int32)
    return code, top * (1.0 / TOP)


def split(values):
    hi = values.astype(jnp.bfloat16)
    return hi, (values - hi.astype(jnp.float32)).astype(jnp.bfloat16)


def whole_kernel(
    slot_in, pos_in, ask_in, owner_in, prolong_in, stiff_ref,
    out_ref,
    slot_ref, pos_ref, ask_ref, owner_ref, prolong_ref,
    meta_ref, mid_ref, req_ref, stage_ref, fetched_ref, mats_ref, pk_ref, cols_ref,
    code_a, code_b, factor_ref, part_a, part_b, scale_ref, table_ref, spread_ref, total_ref,
    rows_a, rows_b, rows_scale, land_a, land_b, land_scale,
    near_send, near_recv, far_send, far_recv, fetch_send, fetch_recv, part_send, part_recv, fact_send, fact_recv,
    rows_send, rows_recv, rsc_send, rsc_recv, mats_sem, req_sem, arg_sem,
):
    n, cv, dof = fetched_ref.shape
    bps = mats_ref.shape[1]
    width = out_ref.shape[2]
    gx, gy = lax.axis_index("gx"), lax.axis_index("gy")
    me = gx * 16 + gy
    z, core = gx // 2, lax.rem(gx, 2)
    x, y = gy // 4, lax.rem(gy, 4)
    to_gy = [lax.rem(x + s // 4, 4) * 4 + lax.rem(y + s % 4, 4) for s in TURNS]
    from_gy = [lax.rem(x + 4 - s // 4, 4) * 4 + lax.rem(y + 4 - s % 4, 4) for s in TURNS]

    def shift(r):
        u = r % 4
        dz = 2 - u + 3 * (u // 2) - 2 * (u // 3)
        other = lax.rem(core + 1 + u % 2 - u // 3 + r // 4, 2)
        return lax.rem(z + dz, 4) * 2 + other, lax.rem(z + 4 - dz, 4) * 2 + other

    def targets(r):
        row, _ = shift(r)
        return [(row, to_gy[s]) for s in range(WIDE)]

    def sources(r):
        _, row = shift(r)
        return [row * 16 + from_gy[s] for s in range(WIDE)]

    def each(fn):
        def body(r, c):
            for where in targets(r):
                fn(r, where)
            return c

        lax.fori_loop(0, ROUNDS - 1, body, 0)
        for where in targets(ROUNDS - 1)[1:]:
            fn(ROUNDS - 1, where)

    def remote(src, dst, send_sem, recv_sem, where):
        return pltpu.make_async_remote_copy(
            src_ref=src, dst_ref=dst, send_sem=send_sem, recv_sem=recv_sem,
            device_id=where, device_id_type=MESH,
        )

    def bulk(src, dst, send_sem, recv_sem, count):
        return remote(
            src.at[pl.ds(0, count)], dst.at[pl.ds(0, count)], send_sem, recv_sem, (gx, gy)
        )

    small = [
        pltpu.make_async_copy(src, dst, arg_sem.at[k])
        for k, (src, dst) in enumerate(
            (
                (ask_in, ask_ref), (pos_in, pos_ref), (slot_in, slot_ref),
                (owner_in, owner_ref), (prolong_in, prolong_ref),
            )
        )
    ]
    for copy in small:
        copy.start()
    loads = [
        pltpu.make_async_copy(
            stiff_ref.at[pl.ds(b * 16, 16)], mats_ref.at[pl.ds(b * 16, 16)], mats_sem.at[b]
        )
        for b in range(n // 16)
    ]
    for copy in loads:
        copy.start()

    barrier = pltpu.get_barrier_semaphore()
    near = [(shift(r)[0], gy) for r in range(ROUNDS - 1)]
    far = [(gx, g) for g in to_gy[1:]]
    for where in near + far:
        pl.semaphore_signal(barrier, inc=1, device_id=where, device_id_type=MESH)

    row_lane = lax.broadcasted_iota(jnp.int32, (1, LANES), 1)

    def describe(h, c):
        for g in range(8):
            p = g * 16 + h
            row = jnp.where(row_lane == 0, ask_ref[p], 0)
            for q in range(bps):
                row = jnp.where(row_lane == 1 + q, pos_ref[q, p], row)
            meta_ref[g, h] = row
        return c

    for copy in small[:2]:
        copy.wait()
    lax.fori_loop(0, 16, describe, 0)
    mid_ref[gx] = meta_ref[gx]
    cols_ref[...] = jnp.zeros_like(cols_ref)
    unit_row = lax.broadcasted_iota(jnp.int32, (SPAN, width), 0)
    unit_col = lax.broadcasted_iota(jnp.int32, (SPAN, width), 1)
    for k in range(MAXNB):
        unit = (unit_row < cv) & (unit_col == unit_row + cv * k)
        table_ref[k] = jnp.where(unit, 1.0, 0.0).astype(jnp.bfloat16)
    pl.semaphore_wait(barrier, 22)
    for where in near:
        remote(
            meta_ref.at[where[0]], mid_ref.at[gx], near_send.at[0], near_recv.at[0], where
        ).start()
    bulk(meta_ref, mid_ref, near_send.at[0], near_recv.at[0], 7).wait()
    for where in far:
        remote(
            mid_ref.at[:, where[1]], req_ref.at[:, gy], far_send.at[0], far_recv.at[0], where
        ).start()
    to_scalars = pltpu.make_async_copy(mid_ref.at[:, gy], req_ref.at[:, gy], req_sem.at[0])
    to_scalars.start()
    remote(
        mid_ref.at[:, pl.ds(0, 15)], req_ref.at[:, pl.ds(0, 15)],
        far_send.at[0], far_recv.at[0], (gx, gy),
    ).wait()
    for copy in small[2:]:
        copy.wait()
    to_scalars.wait()

    def fill(g, c):
        for h in range(16):
            stage_ref[g * 16 + h] = prolong_ref[req_ref[g, h, 0, 0]]
        return c

    lax.fori_loop(0, 8, fill, 0)

    def answer(r, where):
        remote(
            stage_ref.at[where[0] * 16 + where[1]], fetched_ref.at[me],
            fetch_send.at[0], fetch_recv.at[r], where,
        ).start()

    each(answer)
    fetched_ref[me] = prolong_ref[req_ref[gx, gy, 0, 0]]
    for copy in loads:
        copy.wait()

    def left_product(t):
        rows = fetched_ref[t]
        parts = []
        for h in range(bps // 2):
            pair = jnp.concatenate([mats_ref[t, 2 * h], mats_ref[t, 2 * h + 1]], axis=1)
            prod = jnp.dot(rows, pair, preferred_element_type=jnp.float32)
            parts += [prod[:, 0:dof], prod[:, dof : 2 * dof]]
        hi, lo = split(jnp.concatenate(parts, axis=0))
        pk_ref[t, :, 0:dof] = hi
        pk_ref[t, :, dof : 2 * dof] = lo

    def take(r, c):
        bulk(stage_ref, fetched_ref, fetch_send.at[0], fetch_recv.at[r], WIDE).wait_recv()
        for t in sources(r):
            left_product(t)
        return c

    lax.fori_loop(0, ROUNDS - 1, take, 0)
    bulk(
        stage_ref, fetched_ref, fetch_send.at[0], fetch_recv.at[ROUNDS - 1], WIDE - 1
    ).wait_recv()
    for t in sources(ROUNDS - 1):
        left_product(t)

    lane = lax.broadcasted_iota(jnp.int32, (cv, LANES), 1)

    def right_product(t, u):
        for q in range(bps):
            block = fetched_ref[slot_ref[q, t]]
            cols_ref[u, SPAN * q : SPAN * q + cv, 0:dof] = block
            cols_ref[u, SPAN * q : SPAN * q + cv, dof : 2 * dof] = block
        prod = lax.dot_general(pk_ref[t], cols_ref[u], NT, preferred_element_type=jnp.float32)
        one = prod[(bps - 1) * cv :]
        for q in range(bps - 2, -1, -1):
            one = jnp.where(lane < SPAN * (q + 1), prod[q * cv : (q + 1) * cv], one)
        code, factor = coded(one)
        for (first, rows), ref in zip(CHUNKS, (code_a, code_b)):
            ref[t] = code[first : first + rows].astype(jnp.int16)
        factor_ref[t] = as_row(factor)

    def give(where):
        peer = where[0] * 16 + where[1]
        remote(
            factor_ref.at[peer], scale_ref.at[me], fact_send.at[0], fact_recv.at[0], where
        ).start()
        remote(
            code_a.at[peer], part_a.at[me], part_send.at[0], part_recv.at[0], where
        ).start()

    def give_rest(r, where):
        remote(
            code_b.at[where[0] * 16 + where[1]], part_b.at[me],
            part_send.at[1], part_recv.at[1], where,
        ).start()

    def multiply(r):
        for s, where in enumerate(targets(r)):
            right_product(where[0] * 16 + where[1], s % COLS)

    def work(r, c):
        multiply(r)
        for where in targets(r - 1):
            give(where)
        return c

    multiply(0)
    lax.fori_loop(1, ROUNDS, work, 0)
    for where in targets(ROUNDS - 1)[1:]:
        give(where)
    each(give_rest)
    part_a[me] = code_a[me]
    part_b[me] = code_b[me]
    scale_ref[me] = factor_ref[me]

    def locate(g, row):
        for h in range(16):
            row = jnp.where(row_lane == g * 16 + h, owner_ref[req_ref[g, h, 0, 0]], row)
        return row

    place = lax.fori_loop(0, 8, locate, jnp.zeros((1, LANES), jnp.int32))
    hot = jnp.where(
        lax.broadcasted_iota(jnp.int32, (n, LANES), 0) == place, 1.0, 0.0
    ).astype(jnp.bfloat16)
    hot = jnp.concatenate([hot, hot], axis=1)

    tiles = width // LANES

    lane_row = lax.broadcasted_iota(jnp.int32, (1, LANES), 1)
    blocks = [(lane_row + LANES * k) // cv for k in range(tiles)]

    def spread(part, first, rows, g, h):
        d = g * 16 + h
        values = part[d].astype(jnp.int32).astype(jnp.float32)
        values = values * as_column(scale_ref[d], rows, first)
        pos = [req_ref[g, h, 0, 1 + q] for q in range(bps)]
        if h % ROLLED:
            hi = values.astype(jnp.bfloat16).astype(jnp.float32)
            both = jnp.concatenate([hi, values - hi], axis=0).astype(jnp.bfloat16)
            units = jnp.concatenate([table_ref[p] for p in pos], axis=0)
            moved = jnp.dot(both, units, preferred_element_type=jnp.float32)
            moved = moved[:rows] + moved[rows:]
            moved = [moved[:, LANES * k : LANES * (k + 1)] for k in range(tiles)]
        else:
            moved = [jnp.zeros((rows, LANES), jnp.float32)] * tiles
            for q, p in enumerate(pos):
                turned = pltpu.roll(values, lax.rem(p * cv - SPAN * q + LANES, LANES), 1)
                moved = [jnp.where(k == p, turned, m) for k, m in zip(blocks, moved)]
        for k in range(tiles):
            spread_ref[k, pl.ds(d * PITCH + first, rows), :] = moved[k]

    def combine(c, carry):
        at = pl.ds(c, n, stride=PITCH)
        every = jnp.concatenate([spread_ref[k, at, :] for k in range(tiles)], axis=1)
        total = jnp.dot(
            hot, jnp.concatenate(split(every), axis=0), preferred_element_type=jnp.float32
        )
        for k in range(tiles):
            total_ref[k, at, :] = total[:, LANES * k : LANES * (k + 1)]
        return carry

    for h, ((first, rows), code_ref, part, rows_ref, land_ref) in enumerate(
        zip(CHUNKS, (code_a, code_b), (part_a, part_b), (rows_a, rows_b), (land_a, land_b))
    ):
        bulk(code_ref, part, part_send.at[h], part_recv.at[h], n - 1).wait()
        if h == 0:
            bulk(factor_ref, scale_ref, fact_send.at[0], fact_recv.at[0], n - 1).wait()

        def spread_some(g, c):
            for j in range(16):
                spread(part, first, rows, g, j)
            return c

        lax.fori_loop(0, 8, spread_some, 0)
        lax.fori_loop(first, first + rows, combine, 0)

        def encode(o):
            row = jnp.concatenate(
                [total_ref[k, pl.ds(o * PITCH + first, rows), :] for k in range(tiles)], axis=1
            )
            code, factor = coded(row)
            rows_ref[o] = code.astype(jnp.int16)
            rows_scale[h, o] = as_row(factor, first)

        def deliver(r, where):
            peer = where[0] * 16 + where[1]
            remote(
                rows_scale.at[h, peer], land_scale.at[h, me],
                rsc_send.at[h], rsc_recv.at[h, r], where,
            ).start()
            remote(
                rows_ref.at[peer], land_ref.at[me],
                rows_send.at[h], rows_recv.at[h, r], where,
            ).start()

        def encode_all(r):
            for where in targets(r):
                encode(where[0] * 16 + where[1])

        def emit(r, c):
            encode_all(r)
            for where in targets(r - 1):
                deliver(r - 1, where)
            return c

        encode_all(0)
        lax.fori_loop(1, ROUNDS, emit, 0)
        for where in targets(ROUNDS - 1)[1:]:
            deliver(ROUNDS - 1, where)

    for h, ((first, rows), rows_ref, land_ref) in enumerate(
        zip(CHUNKS, (rows_a, rows_b), (land_a, land_b))
    ):
        def decode(code, scale, p):
            out_ref[p, first : first + rows, :] = code.astype(jnp.int32).astype(
                jnp.float32
            ) * as_column(scale, rows, first)

        def arrived(i, count):
            bulk(rows_ref, land_ref, rows_send.at[h], rows_recv.at[h, i], count).wait_recv()
            bulk(
                rows_scale.at[h], land_scale.at[h], rsc_send.at[h], rsc_recv.at[h, i], count
            ).wait_recv()

        decode(rows_ref[me], rows_scale[h, me], me)

        def drain(r, c):
            arrived(r, WIDE)
            for p in sources(r):
                decode(land_ref[p], land_scale[h, p], p)
            return c

        lax.fori_loop(0, ROUNDS - 1, drain, 0)
        arrived(ROUNDS - 1, WIDE - 1)
        for p in sources(ROUNDS - 1)[1:]:
            decode(land_ref[p], land_scale[h, p], p)
        bulk(rows_ref, land_ref, rows_send.at[h], rows_recv.at[h, 0], n - 1).wait_send()
        bulk(
            rows_scale.at[h], land_scale.at[h], rsc_send.at[h], rsc_recv.at[h, 0], n - 1
        ).wait_send()
    bulk(stage_ref, fetched_ref, fetch_send.at[0], fetch_recv.at[0], n - 1).wait_send()


def whole(col_slot, col_pos, request, owners, prolong, stiffness):
    slots, bps, dof, _ = stiffness.shape
    cv = prolong.shape[1]
    n = slots
    width = MAXNB * cv
    sem = pltpu.SemaphoreType.DMA
    bf16, f32, i16, i32 = jnp.bfloat16, jnp.float32, jnp.int16, jnp.int32
    return pl.pallas_call(
        whole_kernel,
        out_shape=jax.ShapeDtypeStruct((n, cv, width), f32),
        in_specs=[HBM] * 6,
        out_specs=VMEM,
        scratch_shapes=[
            pltpu.SMEM(col_slot.shape, i32),
            pltpu.SMEM(col_pos.shape, i32),
            pltpu.SMEM(request.shape, i32),
            pltpu.SMEM(owners.shape, i32),
            pltpu.VMEM(prolong.shape, bf16),
            pltpu.VMEM((8, 16, 1, LANES), i32),
            pltpu.VMEM((8, 16, 1, LANES), i32),
            pltpu.SMEM((8, 16, 1, LANES), i32),
            pltpu.VMEM((n, cv, dof), bf16),
            pltpu.VMEM((n, cv, dof), bf16),
            pltpu.VMEM(stiffness.shape, bf16),
            pltpu.VMEM((n, bps * cv, 2 * dof), bf16),
            pltpu.VMEM((COLS, LANES, 2 * dof), bf16),
            *[pltpu.VMEM((n, rows, LANES), i16) for _, rows in CHUNKS],
            pltpu.VMEM((n, 1, LANES), f32),
            *[pltpu.VMEM((n, rows, LANES), i16) for _, rows in CHUNKS],
            pltpu.VMEM((n, 1, LANES), f32),
            pltpu.VMEM((MAXNB, SPAN, width), bf16),
            pltpu.VMEM((width // LANES, (n + 1) * PITCH, LANES), f32),
            pltpu.VMEM((width // LANES, (n + 1) * PITCH, LANES), f32),
            *[pltpu.VMEM((n, rows, width), i16) for _, rows in CHUNKS],
            pltpu.VMEM((len(CHUNKS), n, 1, LANES), f32),
            *[pltpu.VMEM((n, rows, width), i16) for _, rows in CHUNKS],
            pltpu.VMEM((len(CHUNKS), n, 1, LANES), f32),
            sem((1,)), sem((1,)),
            sem((1,)), sem((1,)),
            sem((1,)), sem((ROUNDS,)),
            sem((2,)), sem((2,)),
            sem((1,)), sem((1,)),
            sem((2,)), sem((2, ROUNDS)),
            sem((2,)), sem((2, ROUNDS)),
            sem((n // 16,)), sem((1,)), sem((5,)),
        ],
        compiler_params=pltpu.CompilerParams(
            collective_id=1, has_side_effects=True, vmem_limit_bytes=46 << 20
        ),
        name="whole",
    )(
        *[
            pltpu.with_memory_space_constraint(a, pltpu.HBM)
            for a in (col_slot, col_pos, request, owners, prolong, stiffness)
        ]
    )


def per_device(prolong, stiffness, request, col_slot, col_pos, coarse_owner):
    return whole(col_slot.T, col_pos.T, request, coarse_owner[:, 0], prolong, stiffness)


def solution(mesh):
    placed = (
        P(AXES, None, None),
        P(AXES, None, None, None),
        P(AXES),
        P(AXES, None),
        P(AXES, None),
        P(AXES, None),
    )
    return jax.shard_map(
        per_device, mesh=mesh, in_specs=placed, out_specs=P(AXES, None, None), check_vma=False
    )
```
